32 devices in a mesh: dp: 8 (over z, y), dap: 4 (over x, core).
Axes of the slice: x: 2, y: 2, z: 4, core: 2. Of those that a mesh axis runs over, the one named last changes fastest.
Arguments:
- single_rep: bfloat16 [8, 128, 384], P('dp', 'dap')
- pair_rep: bfloat16 [8, 128, 128, 128], P('dp', 'dap')
- token_mask: int32 [8, 128], P('dp')
- d_single_out: bfloat16 [8, 128, 384], P('dp', 'dap')
- d_pair_out: bfloat16 [8, 128, 128, 128], P('dp', 'dap')
- mul_out_in: bfloat16 [128, 512], replicated
- mul_out_gate: bfloat16 [128, 128], replicated
- mul_out_proj: bfloat16 [128, 128], replicated
- mul_in_in: bfloat16 [128, 512], replicated
- mul_in_gate: bfloat16 [128, 128], replicated
- mul_in_proj: bfloat16 [128, 128], replicated
- att_st_qkvg: bfloat16 [128, 512], replicated
- att_st_bias: bfloat16 [128, 4], replicated
- att_st_proj: bfloat16 [128, 128], replicated
- att_en_qkvg: bfloat16 [128, 512], replicated
- att_en_bias: bfloat16 [128, 4], replicated
- att_en_proj: bfloat16 [128, 128], replicated
- pair_up: bfloat16 [128, 1024], replicated
- pair_down: bfloat16 [512, 128], replicated
- sing_qkvg: bfloat16 [384, 1536], replicated
- sing_qbias: bfloat16 [384], replicated
- sing_pbias: bfloat16 [128, 16], replicated
- sing_proj: bfloat16 [384, 384], replicated
- sing_up: bfloat16 [384, 3072], replicated
- sing_down: bfloat16 [1536, 384], replicated
Outputs:
- output 1: bfloat16 [8, 128, 384], P('dp', 'dap')
- output 2: bfloat16 [8, 128, 128, 128], P('dp', 'dap')
- output 3: bfloat16 [8, 128, 384], P('dp', 'dap')
- output 4: bfloat16 [8, 128, 128, 128], P('dp', 'dap')
- output 5: float32 [3067264], P('dp')
All inputs are finite; a program needn't handle non-finite values.
Results may differ from the reference program's by a relative error of at most 0.02.
Values are sent between devices in bfloat16 or wider.
A program may use at most 1 GiB of HBM per device.

```python
import jax
import jax.numpy as jnp
from jax import lax

BATCH = 8
TOKENS = 128
C_S = 384
C_Z = 128
HEADS_S = 16
HEAD_S = 24
TRI_HEADS = 4
TRI_HEAD = 32
C_MUL = 128

NORM_EPS = 1e-5
MASK_PENALTY = 1.0e9


def weight_shapes():
    tri_width = TRI_HEADS * TRI_HEAD
    single_width = HEADS_S * HEAD_S
    return [
        ('mul_out_in', (C_Z, 4 * C_MUL), C_Z),
        ('mul_out_gate', (C_Z, C_Z), C_Z),
        ('mul_out_proj', (C_MUL, C_Z), C_MUL),
        ('mul_in_in', (C_Z, 4 * C_MUL), C_Z),
        ('mul_in_gate', (C_Z, C_Z), C_Z),
        ('mul_in_proj', (C_MUL, C_Z), C_MUL),
        ('att_st_qkvg', (C_Z, 4 * tri_width), C_Z),
        ('att_st_bias', (C_Z, TRI_HEADS), C_Z),
        ('att_st_proj', (tri_width, C_Z), tri_width),
        ('att_en_qkvg', (C_Z, 4 * tri_width), C_Z),
        ('att_en_bias', (C_Z, TRI_HEADS), C_Z),
        ('att_en_proj', (tri_width, C_Z), tri_width),
        ('pair_up', (C_Z, 8 * C_Z), C_Z),
        ('pair_down', (4 * C_Z, C_Z), 4 * C_Z),
        ('sing_qkvg', (C_S, 4 * single_width), C_S),
        ('sing_qbias', (single_width,), 1),
        ('sing_pbias', (C_Z, HEADS_S), C_Z),
        ('sing_proj', (single_width, C_S), single_width),
        ('sing_up', (C_S, 8 * C_S), C_S),
        ('sing_down', (4 * C_S, C_S), 4 * C_S),
    ]


def setup_inputs(seed: int = 0) -> dict:
    base_key = jax.random.key(seed)
    key_list = jax.random.split(base_key, 32)
    lengths = jax.random.randint(key_list[0], (BATCH,), TOKENS // 4, TOKENS + 1)
    full_pick = jax.random.randint(key_list[1], (), 0, BATCH)
    lengths = jnp.where(jnp.arange(BATCH) == full_pick, TOKENS, lengths)
    inputs = {}
    inputs['single_rep'] = jax.random.normal(key_list[2], (BATCH, TOKENS, C_S), jnp.float32).astype(jnp.bfloat16)
    inputs['pair_rep'] = jax.random.normal(key_list[3], (BATCH, TOKENS, TOKENS, C_Z), jnp.float32).astype(jnp.bfloat16)
    inputs['token_mask'] = (jnp.arange(TOKENS)[None, :] < lengths[:, None]).astype(jnp.int32)
    inputs['d_single_out'] = jax.random.normal(key_list[4], (BATCH, TOKENS, C_S), jnp.float32).astype(jnp.bfloat16)
    inputs['d_pair_out'] = jax.random.normal(key_list[5], (BATCH, TOKENS, TOKENS, C_Z), jnp.float32).astype(jnp.bfloat16)
    for w_index, (w_name, w_shape, fan_in) in enumerate(weight_shapes()):
        w_draw = jax.random.normal(key_list[6 + w_index], w_shape, jnp.float32)
        inputs[w_name] = (w_draw * fan_in ** -0.5).astype(jnp.bfloat16)
    return inputs


def layer_norm(x_in):
    x_f32 = x_in.astype(jnp.float32)
    centered = x_f32 - jnp.mean(x_f32, axis=-1, keepdims=True)
    row_var = jnp.mean(centered * centered, axis=-1, keepdims=True)
    return centered * lax.rsqrt(row_var + NORM_EPS)


def tri_mul(z_one, w_in, w_gate, w_out, mix_form):
    normed = layer_norm(z_one).astype(jnp.bfloat16)
    proj_all = jnp.dot(normed, w_in, preferred_element_type=jnp.float32)
    left_proj = (jax.nn.sigmoid(proj_all[..., C_MUL:2 * C_MUL]) * proj_all[..., :C_MUL]).astype(jnp.bfloat16)
    right_proj = (jax.nn.sigmoid(proj_all[..., 3 * C_MUL:]) * proj_all[..., 2 * C_MUL:3 * C_MUL]).astype(jnp.bfloat16)
    gate_vals = jax.nn.sigmoid(jnp.dot(normed, w_gate, preferred_element_type=jnp.float32))
    mixed_sum = jnp.einsum(mix_form, left_proj.astype(jnp.float32), right_proj.astype(jnp.float32))
    mixed_norm = layer_norm(mixed_sum).astype(jnp.bfloat16)
    update = gate_vals * jnp.dot(mixed_norm, w_out, preferred_element_type=jnp.float32)
    return (z_one.astype(jnp.float32) + update).astype(jnp.bfloat16)


def tri_att(z_one, mask_bias, w_qkvg, w_tb, w_o):
    normed = layer_norm(z_one).astype(jnp.bfloat16)
    proj_all = jnp.dot(normed, w_qkvg, preferred_element_type=jnp.float32)
    tri_width = TRI_HEADS * TRI_HEAD
    head_shape = (TOKENS, TOKENS, TRI_HEADS, TRI_HEAD)
    q_all = proj_all[..., :tri_width].astype(jnp.bfloat16).reshape(head_shape)
    k_all = proj_all[..., tri_width:2 * tri_width].astype(jnp.bfloat16).reshape(head_shape)
    v_all = proj_all[..., 2 * tri_width:3 * tri_width].astype(jnp.bfloat16).reshape(head_shape)
    gate_vals = jax.nn.sigmoid(proj_all[..., 3 * tri_width:])
    bias_hjk = jnp.transpose(jnp.dot(normed, w_tb, preferred_element_type=jnp.float32).astype(jnp.bfloat16), (2, 0, 1)).astype(jnp.float32)
    att_scale = TRI_HEAD ** -0.5

    def one_row(row_item):
        q_row, k_row, v_row = row_item
        logits = jnp.einsum('jhd,khd->hjk', q_row.astype(jnp.float32), k_row.astype(jnp.float32)) * att_scale + bias_hjk + mask_bias
        prob_mat = jax.nn.softmax(logits, axis=-1).astype(jnp.bfloat16)
        return jnp.einsum('hjk,khd->jhd', prob_mat.astype(jnp.float32), v_row.astype(jnp.float32))

    attended = lax.map(one_row, (q_all, k_all, v_all))
    gated = (gate_vals * attended.reshape(TOKENS, TOKENS, tri_width)).astype(jnp.bfloat16)
    return (z_one.astype(jnp.float32) + jnp.dot(gated, w_o, preferred_element_type=jnp.float32)).astype(jnp.bfloat16)


def transition(x_rows, w_up, w_down):
    normed = layer_norm(x_rows).astype(jnp.bfloat16)
    hidden = jnp.dot(normed, w_up, preferred_element_type=jnp.float32)
    inner_dim = w_down.shape[0]
    acted = (jax.nn.silu(hidden[..., :inner_dim]) * hidden[..., inner_dim:]).astype(jnp.bfloat16)
    return (x_rows.astype(jnp.float32) + jnp.dot(acted, w_down, preferred_element_type=jnp.float32)).astype(jnp.bfloat16)


def single_att(s_one, z_one, mask_bias, w_qkvg, q_bias, w_pb, w_o):
    normed = layer_norm(s_one).astype(jnp.bfloat16)
    proj_all = jnp.dot(normed, w_qkvg, preferred_element_type=jnp.float32)
    single_width = HEADS_S * HEAD_S
    head_shape = (TOKENS, HEADS_S, HEAD_S)
    q_all = (proj_all[:, :single_width] + q_bias.astype(jnp.float32)).astype(jnp.bfloat16).reshape(head_shape)
    k_all = proj_all[:, single_width:2 * single_width].astype(jnp.bfloat16).reshape(head_shape)
    v_all = proj_all[:, 2 * single_width:3 * single_width].astype(jnp.bfloat16).reshape(head_shape)
    gate_vals = jax.nn.sigmoid(proj_all[:, 3 * single_width:])
    pair_norm = layer_norm(z_one).astype(jnp.bfloat16)
    bias_all = jnp.dot(pair_norm, w_pb, preferred_element_type=jnp.float32).astype(jnp.bfloat16)
    logits = jnp.einsum('ihd,jhd->hij', q_all.astype(jnp.float32), k_all.astype(jnp.float32)) * HEAD_S ** -0.5
    logits = logits + jnp.transpose(bias_all, (2, 0, 1)).astype(jnp.float32) + mask_bias
    prob_mat = jax.nn.softmax(logits, axis=-1).astype(jnp.bfloat16)
    attended = jnp.einsum('hij,jhd->ihd', prob_mat.astype(jnp.float32), v_all.astype(jnp.float32))
    gated = (gate_vals * attended.reshape(TOKENS, single_width)).astype(jnp.bfloat16)
    return (s_one.astype(jnp.float32) + jnp.dot(gated, w_o, preferred_element_type=jnp.float32)).astype(jnp.bfloat16)


def block_forward(s_one, z_one, mask_one, params):
    w_list = [p_item.astype(jnp.bfloat16) for p_item in params]
    mask_bias = (mask_one.astype(jnp.float32) - 1.0) * MASK_PENALTY
    z_val = tri_mul(z_one, w_list[0], w_list[1], w_list[2], 'ikc,jkc->ijc')
    z_val = tri_mul(z_val, w_list[3], w_list[4], w_list[5], 'kic,kjc->ijc')
    z_val = tri_att(z_val, mask_bias, w_list[6], w_list[7], w_list[8])
    z_val = jnp.transpose(tri_att(jnp.transpose(z_val, (1, 0, 2)), mask_bias, w_list[9], w_list[10], w_list[11]), (1, 0, 2))
    z_val = transition(z_val, w_list[12], w_list[13])
    s_val = single_att(s_one, z_val, mask_bias, w_list[14], w_list[15], w_list[16], w_list[17])
    s_val = transition(s_val, w_list[18], w_list[19])
    return s_val, z_val


def reference(single_rep, pair_rep, token_mask, d_single_out, d_pair_out, mul_out_in, mul_out_gate, mul_out_proj, mul_in_in, mul_in_gate, mul_in_proj, att_st_qkvg, att_st_bias, att_st_proj, att_en_qkvg, att_en_bias, att_en_proj, pair_up, pair_down, sing_qkvg, sing_qbias, sing_pbias, sing_proj, sing_up, sing_down):
    weights = (mul_out_in, mul_out_gate, mul_out_proj, mul_in_in, mul_in_gate, mul_in_proj, att_st_qkvg, att_st_bias, att_st_proj, att_en_qkvg, att_en_bias, att_en_proj, pair_up, pair_down, sing_qkvg, sing_qbias, sing_pbias, sing_proj, sing_up, sing_down)
    params = tuple(w_item.astype(jnp.float32) for w_item in weights)

    def scan_step(grad_acc, scan_item):
        s_one, z_one, mask_one, gs_one, gz_one = scan_item

        def forward_one(s_val, z_val, p_val):
            return block_forward(s_val, z_val, mask_one, p_val)

        outs_one, pull_back = jax.vjp(forward_one, s_one, z_one, params)
        ds_one, dz_one, grad_one = pull_back((gs_one, gz_one))
        new_acc = tuple(acc_item + grad_item for acc_item, grad_item in zip(grad_acc, grad_one))
        return new_acc, (outs_one[0], outs_one[1], ds_one, dz_one)

    init_acc = tuple(jnp.zeros_like(p_item) for p_item in params)
    grad_sums, stacked = lax.scan(scan_step, init_acc, (single_rep, pair_rep, token_mask, d_single_out, d_pair_out))
    grad_flat = jnp.concatenate([g_item.reshape(-1) for g_item in grad_sums])
    return stacked[0], stacked[1], stacked[2], stacked[3], grad_flat
```

```python
import functools
import jax
import jax.numpy as jnp
from jax import lax
from jax.experimental import pallas as pl
from jax.experimental.pallas import tpu as pltpu
from jax.sharding import PartitionSpec as P

BATCH_AXIS = 'dp'
GROUP_AXIS = 'dap'
NORM_EPS = 1e-5
MASK_PENALTY = 1.0e9
ROWS_STEP = 4
CHAN_STEP = 8
INTERPRET = False
BF16 = jnp.bfloat16
F32 = jnp.float32


def nn(x, y):
    return lax.dot_general(x, y, (((1,), (0,)), ((), ())), preferred_element_type=F32)


def nt(x, y):
    return lax.dot_general(x, y, (((1,), (1,)), ((), ())), preferred_element_type=F32)


def tn(x, y):
    return lax.dot_general(x, y, (((0,), (0,)), ((), ())), preferred_element_type=F32)


def norm_parts(x):
    xf = x.astype(F32)
    cent = xf - jnp.mean(xf, axis=-1, keepdims=True)
    rstd = lax.rsqrt(jnp.mean(cent * cent, axis=-1, keepdims=True) + NORM_EPS)
    return cent * rstd, rstd


def norm_back(xhat, rstd, dn):
    m1 = jnp.mean(dn, axis=-1, keepdims=True)
    m2 = jnp.mean(dn * xhat, axis=-1, keepdims=True)
    return rstd * (dn - m1 - xhat * m2)


def round_bf(x):
    return x.astype(BF16).astype(F32)


def swap_lead(src, dst):
    steps = src.shape[1] // 16

    def body(t, carry):
        at = pl.ds(pl.multiple_of(t * 16, 16), 16)
        dst[at] = jnp.swapaxes(src[:, at, :], 0, 1)
        return carry
    lax.fori_loop(0, steps, body, 0)


def swap_minor(src, dst, step=4):
    def body(t, carry):
        at = pl.ds(t * step, step)
        dst[at] = jnp.swapaxes(src[at], 1, 2)
        return carry
    lax.fori_loop(0, src.shape[0] // step, body, 0)


def rows_loop(count, body):
    def wrapped(t, carry):
        body(t)
        return carry
    lax.fori_loop(0, count, wrapped, 0)


def call(body, outs, scratch, *args, name):
    outs = [jax.ShapeDtypeStruct(s, d) for s, d in outs]
    return pl.pallas_call(
        body, out_shape=outs, scratch_shapes=scratch, name=name, interpret=INTERPRET,
        in_specs=[pl.BlockSpec(memory_space=pltpu.VMEM)] * len(args),
        out_specs=[pl.BlockSpec(memory_space=pltpu.VMEM)] * len(outs),
        compiler_params=pltpu.CompilerParams(vmem_limit_bytes=56 * 1024 * 1024),
    )(*args)


def mul_pre_body(keep_left, z, w_in, *refs):
    if keep_left:
        left_t, right_t, left_nat, sa, sb = refs
    else:
        left_t, right_t, sa, sb = refs
    width = w_in.shape[1] // 4

    def step(t):
        at = pl.ds(t * ROWS_STEP, ROWS_STEP)
        zc = z[at].reshape(-1, z.shape[-1])
        normed = norm_parts(zc)[0].astype(BF16)
        proj = nn(normed, w_in[...])
        left = (jax.nn.sigmoid(proj[:, width:2 * width]) * proj[:, :width]).astype(BF16)
        right = (jax.nn.sigmoid(proj[:, 3 * width:]) * proj[:, 2 * width:3 * width]).astype(BF16)
        left = left.reshape(ROWS_STEP, -1, width)
        right = right.reshape(ROWS_STEP, -1, width)
        if keep_left:
            left_nat[at] = left
        sa[at] = jnp.swapaxes(left, 1, 2)
        sb[at] = jnp.swapaxes(right, 1, 2)
    rows_loop(z.shape[0] // ROWS_STEP, step)
    swap_lead(sa, left_t)
    swap_lead(sb, right_t)


def mul_pre(z, w_in, keep_left):
    r, n, c = z.shape
    width = w_in.shape[1] // 4
    outs = [((width, r, n), BF16)] * 2 + ([((r, n, width), BF16)] if keep_left else [])
    scratch = [pltpu.VMEM((r, width, n), BF16)] * 2
    return call(functools.partial(mul_pre_body, keep_left), outs, scratch, z, w_in,
                name='mul_pre_in' if keep_left else 'mul_pre_out')


def joined(ref, ch):
    return jnp.concatenate([ref[dev, ch] for dev in range(ref.shape[0])], axis=0)


def mul_post_body(incoming, left, right_g, z, w_gate, w_out, w_tb, z_new, xh_nat, xhat, rstd, bias, *scr):
    tb, t2 = scr[0], scr[1]
    width = xhat.shape[0]
    if incoming:
        u1, u2, u3 = scr[2], scr[3], scr[4]
        swap_lead(left, u1)
        swap_minor(u1, u2)
        swap_lead(u2, u3)
        left = u3

    def mix(t):
        for s in range(CHAN_STEP):
            ch = t * CHAN_STEP + s
            if incoming:
                xhat[ch] = nn(left[ch], joined(right_g, ch))
            else:
                xhat[ch] = nt(left[ch], joined(right_g, ch))
    rows_loop(width // CHAN_STEP, mix)
    zero = jnp.zeros(xhat.shape[1:], F32)
    total = lax.fori_loop(0, width, lambda ch, acc: acc + xhat[ch], zero)
    mean = total / width
    sq = lax.fori_loop(0, width, lambda ch, acc: acc + (xhat[ch] - mean) * (xhat[ch] - mean), zero)
    inv = lax.rsqrt(sq / width + NORM_EPS)
    rstd[...] = inv

    def scale(ch):
        val = (xhat[ch] - mean) * inv
        xhat[ch] = val
        tb[ch] = val.astype(BF16)
    rows_loop(width, scale)
    swap_lead(tb, t2)

    def step(t):
        at = pl.ds(t * ROWS_STEP, ROWS_STEP)
        zc = z[at].reshape(-1, z.shape[-1])
        xh = jnp.swapaxes(t2[at], 1, 2)
        xh_nat[at] = xh
        normed = norm_parts(zc)[0].astype(BF16)
        gate = jax.nn.sigmoid(nn(normed, w_gate[...]))
        upd = gate * nn(xh.reshape(-1, width), w_out[...])
        znew = (zc.astype(F32) + upd).astype(BF16)
        z_new[at] = znew.reshape(ROWS_STEP, -1, z.shape[-1])
        if incoming:
            bias_rows(znew, w_tb, bias, t)
    rows_loop(z.shape[0] // ROWS_STEP, step)
    if not incoming:
        bias[...] = jnp.zeros_like(bias)


def bias_rows(zc, w_t, bias, t):
    normed = norm_parts(zc)[0].astype(BF16).reshape(ROWS_STEP, -1, zc.shape[-1])
    for s in range(ROWS_STEP):
        bias[t * ROWS_STEP + s] = nt(w_t[...], normed[s]).astype(BF16)


def mul_post(left, right_g, z, w_gate, w_out, w_tb, incoming):
    r, n, c = z.shape
    width = w_out.shape[0]
    outs = [((r, n, c), BF16), ((r, n, width), BF16), ((width, r, n), F32), ((r, n), F32), ((r, 16, n), BF16)]
    scratch = [pltpu.VMEM((width, r, n), BF16), pltpu.VMEM((r, width, n), BF16)]
    if incoming:
        scratch += [pltpu.VMEM((r, n, width), BF16), pltpu.VMEM((r, width, n), BF16), pltpu.VMEM((width, r, n), BF16)]
    return call(functools.partial(mul_post_body, incoming), outs, scratch, left, right_g, z, w_gate, w_out, w_tb,
                name='mul_post_in' if incoming else 'mul_post_out')


def mul_back_post_body(want_nat, dz, z, xh_nat, xhat, rstd, w_gate, w_out, d_t, dgp, g_out, *refs):
    if want_nat:
        d_nat, td, td2 = refs
    else:
        td, td2 = refs
    width = xhat.shape[0]
    g_out[...] = jnp.zeros_like(g_out)

    def step(t):
        at = pl.ds(t * ROWS_STEP, ROWS_STEP)
        zc = z[at].reshape(-1, z.shape[-1])
        dzf = dz[at].reshape(-1, z.shape[-1]).astype(F32)
        xh = xh_nat[at].reshape(-1, width)
        normed = norm_parts(zc)[0].astype(BF16)
        gate = jax.nn.sigmoid(nn(normed, w_gate[...]))
        y = nn(xh, w_out[...])
        dgp[at] = (dzf * y * gate * (1.0 - gate)).astype(BF16).reshape(ROWS_STEP, -1, z.shape[-1])
        dy = (dzf * gate).astype(BF16)
        g_out[...] += tn(xh, dy)
        dxh = nt(dy, w_out[...]).astype(BF16).reshape(ROWS_STEP, -1, width)
        td[at] = jnp.swapaxes(dxh, 1, 2)
    rows_loop(z.shape[0] // ROWS_STEP, step)
    swap_lead(td, td2)
    zero = jnp.zeros(xhat.shape[1:], F32)

    def sums(ch, acc):
        d = td2[ch].astype(F32)
        return acc[0] + d, acc[1] + d * xhat[ch]
    s1, s2 = lax.fori_loop(0, width, sums, (zero, zero))
    s1, s2, inv = s1 / width, s2 / width, rstd[...]

    def fin(ch):
        d_t[ch] = (inv * (td2[ch].astype(F32) - s1 - xhat[ch] * s2)).astype(BF16)
    rows_loop(width, fin)
    if want_nat:
        swap_lead(d_t, td)
        swap_minor(td, d_nat)


def mul_back_post(dz, z, xh_nat, xhat, rstd, w_gate, w_out, want_nat):
    r, n, c = z.shape
    width = w_out.shape[0]
    outs = [((width, r, n), BF16), ((r, n, c), BF16), ((width, c), F32)]
    if want_nat:
        outs.append(((r, n, width), BF16))
    scratch = [pltpu.VMEM((r, width, n), BF16), pltpu.VMEM((width, r, n), BF16)]
    return call(functools.partial(mul_back_post_body, want_nat), outs, scratch, dz, z, xh_nat, xhat, rstd, w_gate, w_out,
                name='mul_back_post')


def mul_back_pre_body(incoming, dz, z, dgp, opa, opb, opc, opd, w_in, w_gate, dz_in, g_in, g_gate, da_t, db_t, da_r, db_r,
                      *scr):
    width = w_in.shape[1] // 4
    if incoming:
        d_g, left_t, right_t = opa, opb, opc
    else:
        d_t, d_recv, right_g, left_g = opa, opb, opc, opd
        u1, u2, u3 = scr
        swap_lead(d_recv, u1)
        swap_minor(u1, u2)
        swap_lead(u2, u3)

    def mix(t):
        for s in range(CHAN_STEP):
            ch = t * CHAN_STEP + s
            if incoming:
                d_all = joined(d_g, ch)
                da_t[ch] = nt(right_t[ch], d_all).astype(BF16)
                db_t[ch] = nn(left_t[ch], d_all).astype(BF16)
            else:
                da_t[ch] = nn(d_t[ch], joined(right_g, ch)).astype(BF16)
                db_t[ch] = nn(u3[ch], joined(left_g, ch)).astype(BF16)
    rows_loop(width // CHAN_STEP, mix)
    swap_lead(da_t, da_r)
    swap_lead(db_t, db_r)
    g_in[...] = jnp.zeros_like(g_in)
    g_gate[...] = jnp.zeros_like(g_gate)

    def step(t):
        at = pl.ds(t * ROWS_STEP, ROWS_STEP)
        c = z.shape[-1]
        zc = z[at].reshape(-1, c)
        da = jnp.swapaxes(da_r[at], 1, 2).reshape(-1, width).astype(F32)
        db = jnp.swapaxes(db_r[at], 1, 2).reshape(-1, width).astype(F32)
        zhat, inv = norm_parts(zc)
        normed = zhat.astype(BF16)
        proj = nn(normed, w_in[...])
        sa = jax.nn.sigmoid(proj[:, width:2 * width])
        sb = jax.nn.sigmoid(proj[:, 3 * width:])
        dproj = jnp.concatenate([
            (da * sa).astype(BF16), (da * proj[:, :width] * sa * (1.0 - sa)).astype(BF16),
            (db * sb).astype(BF16), (db * proj[:, 2 * width:3 * width] * sb * (1.0 - sb)).astype(BF16)], axis=1)
        dg = dgp[at].reshape(-1, c)
        g_in[...] += tn(normed, dproj)
        g_gate[...] += tn(normed, dg)
        dn = round_bf(nt(dproj, w_in[...]) + nt(dg, w_gate[...]))
        out = dz[at].reshape(-1, c).astype(F32) + norm_back(zhat, inv, dn)
        dz_in[at] = out.astype(BF16).reshape(ROWS_STEP, -1, c)
    rows_loop(z.shape[0] // ROWS_STEP, step)


def mul_back_pre(dz, z, dgp, opa, opb, opc, opd, w_in, w_gate, incoming):
    r, n, c = z.shape
    width = w_in.shape[1] // 4
    outs = [((r, n, c), BF16), (w_in.shape, F32), (w_gate.shape, F32)]
    scratch = [pltpu.VMEM((width, r, n), BF16)] * 2 + [pltpu.VMEM((r, width, n), BF16)] * 2
    if not incoming:
        scratch += [pltpu.VMEM((r, n, width), BF16), pltpu.VMEM((r, width, n), BF16), pltpu.VMEM((width, r, n), BF16)]
    return call(functools.partial(mul_back_pre_body, incoming), outs, scratch, dz, z, dgp, opa, opb, opc, opd, w_in, w_gate,
                name='mul_back_pre_in' if incoming else 'mul_back_pre_out')


def head_masks(width, heads):
    lane = lax.broadcasted_iota(jnp.int32, (1, width), 1)
    size = width // heads
    return [(lane >= h * size) & (lane < (h + 1) * size) for h in range(heads)]


def stack_heads(x, masks):
    zero = jnp.zeros_like(x)
    return jnp.concatenate([jnp.where(m, x, zero) for m in masks], axis=0)


def pick_heads(x, masks):
    n = x.shape[0] // len(masks)
    out = x[:n]
    for h in range(1, len(masks)):
        out = jnp.where(masks[h], x[h * n:(h + 1) * n], out)
    return out


def load_bias(bias_g, bias_s, add_mask, heads):
    n = bias_g.shape[0]
    for h in range(heads):
        bias_s[h * n:(h + 1) * n] = bias_g[:, h, :].astype(F32) + add_mask


def soft(logits):
    top = jnp.max(logits, axis=-1, keepdims=True)
    e = jnp.exp(logits - top)
    return e / jnp.sum(e, axis=-1, keepdims=True)


def att_body(heads, z, bias_g, mask, w_qkvg, w_o, z_new, bias_s):
    width = w_o.shape[0]
    n = z.shape[1]
    masks = head_masks(width, heads)
    scale = (width // heads) ** -0.5
    load_bias(bias_g, bias_s, mask[...], heads)

    def step(t):
        at = pl.ds(t * ROWS_STEP, ROWS_STEP)
        zc = z[at].reshape(-1, z.shape[-1])
        normed = norm_parts(zc)[0].astype(BF16)
        proj = nn(normed, w_qkvg[...])
        qkv = proj[:, :3 * width].astype(BF16)
        outs = []
        for s in range(ROWS_STEP):
            row = qkv[s * n:(s + 1) * n]
            q, k, v = row[:, :width], row[:, width:2 * width], row[:, 2 * width:]
            prob = soft(nt(stack_heads(q, masks), k) * scale + bias_s[...]).astype(BF16)
            outs.append(pick_heads(nn(prob, v), masks))
        att = jnp.concatenate(outs, axis=0)
        gated = (jax.nn.sigmoid(proj[:, 3 * width:]) * att).astype(BF16)
        out = (zc.astype(F32) + nn(gated, w_o[...])).astype(BF16)
        z_new[at] = out.reshape(ROWS_STEP, n, -1)
    rows_loop(z.shape[0] // ROWS_STEP, step)


def att_fwd(z, bias_g, mask, w_qkvg, w_o, heads):
    n = z.shape[1]
    return call(functools.partial(att_body, heads), [(z.shape, BF16)], [pltpu.VMEM((heads * n, n), F32)],
                z, bias_g, mask, w_qkvg, w_o, name='att_fwd')[0]


def att_back_body(heads, dz, z, bias_g, mask, w_qkvg, w_o, dz_part, d_bias, g_qkvg, g_o, bias_s):
    width = w_o.shape[0]
    n, c = z.shape[1:]
    masks = head_masks(width, heads)
    scale = (width // heads) ** -0.5
    load_bias(bias_g, bias_s, mask[...], heads)
    d_bias[...] = jnp.zeros_like(d_bias)
    g_qkvg[...] = jnp.zeros_like(g_qkvg)
    g_o[...] = jnp.zeros_like(g_o)
    step_rows = 2

    def step(t):
        at = pl.ds(t * step_rows, step_rows)
        zc = z[at].reshape(-1, c)
        dzc = dz[at].reshape(-1, c)
        zhat, inv = norm_parts(zc)
        normed = zhat.astype(BF16)
        proj = nn(normed, w_qkvg[...])
        qkv = proj[:, :3 * width].astype(BF16)
        gate = jax.nn.sigmoid(proj[:, 3 * width:])
        d_gated = round_bf(nt(dzc, w_o[...]))
        d_att = (d_gated * gate).astype(BF16)
        atts, dprojs = [], []
        for s in range(step_rows):
            row = qkv[s * n:(s + 1) * n]
            q, k, v = row[:, :width], row[:, width:2 * width], row[:, 2 * width:]
            qs = stack_heads(q, masks)
            prob = soft(nt(qs, k) * scale + bias_s[...])
            prob_b = prob.astype(BF16)
            att = pick_heads(nn(prob_b, v), masks)
            das = stack_heads(d_att[s * n:(s + 1) * n], masks)
            dp = round_bf(nt(das, v))
            ds = prob * (dp - jnp.sum(prob * dp, axis=-1, keepdims=True))
            d_bias[...] += ds
            dsb = (ds * scale).astype(BF16)
            dq = pick_heads(nn(dsb, k), masks)
            dk = tn(dsb, qs)
            dv = tn(prob_b, das)
            atts.append(att)
            dprojs.append(jnp.concatenate([dq.astype(BF16), dk.astype(BF16), dv.astype(BF16)], axis=1))
        att = jnp.concatenate(atts, axis=0)
        d_gl = (d_gated * att * gate * (1.0 - gate)).astype(BF16)
        gated = (gate * att).astype(BF16)
        dproj = jnp.concatenate([jnp.concatenate(dprojs, axis=0), d_gl], axis=1)
        g_o[...] += tn(gated, dzc)
        g_qkvg[...] += tn(normed, dproj)
        dn = round_bf(nt(dproj, w_qkvg[...]))
        out = dzc.astype(F32) + norm_back(zhat, inv, dn)
        dz_part[at] = out.reshape(step_rows, n, c)
    rows_loop(z.shape[0] // step_rows, step)


def att_back(dz, z, bias_g, mask, w_qkvg, w_o, heads):
    n = z.shape[1]
    outs = [(z.shape, F32), ((heads * n, n), F32), (w_qkvg.shape, F32), (w_o.shape, F32)]
    return call(functools.partial(att_back_body, heads), outs, [pltpu.VMEM((heads * n, n), F32)],
                dz, z, bias_g, mask, w_qkvg, w_o, name='att_back')


def bias_back_rows(zc, db, w_t, g_t, t):
    zhat, inv = norm_parts(zc)
    normed = zhat.astype(BF16).reshape(ROWS_STEP, -1, zc.shape[-1])
    dns = []
    for s in range(ROWS_STEP):
        d = db[t * ROWS_STEP + s]
        dns.append(tn(d, w_t[...]))
        g_t[...] += nn(d, normed[s])
    return norm_back(zhat, inv, round_bf(jnp.concatenate(dns, axis=0)))


def bias_back_body(swap_out, dz_part, z, db, w_t, dz, g_t, *scr):
    g_t[...] = jnp.zeros_like(g_t)
    dst = scr[0] if swap_out else dz

    def step(t):
        at = pl.ds(t * ROWS_STEP, ROWS_STEP)
        c = z.shape[-1]
        add = bias_back_rows(z[at].reshape(-1, c), db, w_t, g_t, t)
        dst[at] = (dz_part[at].reshape(-1, c) + add).astype(BF16).reshape(ROWS_STEP, -1, c)
    rows_loop(z.shape[0] // ROWS_STEP, step)
    if swap_out:
        swap_lead(scr[0], dz)


def bias_back(dz_part, z, db, w_t, swap_out):
    r, n, c = z.shape
    out = (n, r, c) if swap_out else (r, n, c)
    scratch = [pltpu.VMEM((r, n, c), BF16)] if swap_out else []
    return call(functools.partial(bias_back_body, swap_out), [(out, BF16), (w_t.shape, F32)], scratch,
                dz_part, z, db, w_t, name='bias_back')


def turn_body(recv, w_t, z_cols, bias):
    swap_lead(recv, z_cols)

    def step(t):
        zc = z_cols[pl.ds(t * ROWS_STEP, ROWS_STEP)].reshape(-1, z_cols.shape[-1])
        bias_rows(zc, w_t, bias, t)
    rows_loop(z_cols.shape[0] // ROWS_STEP, step)


def turn(recv, w_t):
    n, r, c = recv.shape
    return call(turn_body, [((r, n, c), BF16), ((r, 16, n), BF16)], [], recv, w_t, name='turn')


def pair_trans_body(z, w_up, w_down, w_t, z_new, z_turn, bias):
    inner = w_down.shape[0]

    def step(t):
        at = pl.ds(t * ROWS_STEP, ROWS_STEP)
        zc = z[at].reshape(-1, z.shape[-1])
        normed = norm_parts(zc)[0].astype(BF16)
        hid = nn(normed, w_up[...])
        acted = (jax.nn.silu(hid[:, :inner]) * hid[:, inner:]).astype(BF16)
        out = (zc.astype(F32) + nn(acted, w_down[...])).astype(BF16)
        z_new[at] = out.reshape(ROWS_STEP, -1, z.shape[-1])
        bias_rows(out, w_t, bias, t)
    rows_loop(z.shape[0] // ROWS_STEP, step)
    swap_lead(z_new, z_turn)


def pair_trans(z, w_up, w_down, w_t):
    r, n, c = z.shape
    return call(pair_trans_body, [((r, n, c), BF16), ((n, r, c), BF16), ((r, 16, n), BF16)], [],
                z, w_up, w_down, w_t, name='pair_trans')


def silu_parts(h1, h2):
    sg = jax.nn.sigmoid(h1)
    return sg, h1 * sg


def pair_trans_back_body(d_recv, z5, db, z, w_up, w_down, w_t, dz_in, g_up, g_down, g_t, dz5):
    inner = w_down.shape[0]
    g_up[...] = jnp.zeros_like(g_up)
    g_down[...] = jnp.zeros_like(g_down)
    g_t[...] = jnp.zeros_like(g_t)
    swap_lead(d_recv, dz5)

    def step(t):
        at = pl.ds(t * ROWS_STEP, ROWS_STEP)
        c = z.shape[-1]
        add = bias_back_rows(z5[at].reshape(-1, c), db, w_t, g_t, t)
        dzc = (dz5[at].reshape(-1, c).astype(F32) + add).astype(BF16)
        zhat, inv = norm_parts(z[at].reshape(-1, c))
        normed = zhat.astype(BF16)
        hid = nn(normed, w_up[...])
        h1, h2 = hid[:, :inner], hid[:, inner:]
        sg, si = silu_parts(h1, h2)
        acted = (si * h2).astype(BF16)
        d_act = round_bf(nt(dzc, w_down[...]))
        d1 = (d_act * h2 * (sg + si * (1.0 - sg))).astype(BF16)
        d2 = (d_act * si).astype(BF16)
        dh = jnp.concatenate([d1, d2], axis=1)
        g_down[...] += tn(acted, dzc)
        g_up[...] += tn(normed, dh)
        dn = round_bf(nt(dh, w_up[...]))
        out = dzc.astype(F32) + norm_back(zhat, inv, dn)
        dz_in[at] = out.astype(BF16).reshape(ROWS_STEP, -1, c)
    rows_loop(z.shape[0] // ROWS_STEP, step)


def pair_trans_back(d_recv, z5, db, z, w_up, w_down, w_t):
    r, n, c = z.shape
    outs = [((r, n, c), BF16), (w_up.shape, F32), (w_down.shape, F32), (w_t.shape, F32)]
    return call(pair_trans_back_body, outs, [pltpu.VMEM((r, n, c), BF16)], d_recv, z5, db, z, w_up, w_down, w_t,
                name='pair_trans_back')


def put_rows(out, first, blocks, block, value):
    out[pl.ds(first + block, value.shape[0], stride=blocks), :] = value


def single_body(heads, s, ds, pb_g, mask_col, w_qkvg, q_bias, w_o, w_up, w_down, s_new, ds_in, d_pb, grads,
                pb_t, probs, acc_a, acc_b, acc_c, dh_s, act_s):
    c = s.shape[1]
    n = s.shape[0]
    inner = w_down.shape[0]
    size = c // heads
    scale = size ** -0.5
    lane = lax.broadcasted_iota(jnp.int32, (1, c), 1)
    swap_lead(pb_g, pb_t)

    def masked(x, h):
        return jnp.where((lane >= h * size) & (lane < (h + 1) * size), x, jnp.zeros_like(x))

    s_hat, s_inv = norm_parts(s[...])
    normed = s_hat.astype(BF16)
    proj = nn(normed, w_qkvg[...])
    q = (proj[:, :c] + q_bias[...].astype(F32)).astype(BF16)
    k = proj[:, c:2 * c].astype(BF16)
    v = proj[:, 2 * c:3 * c].astype(BF16)
    gate = jax.nn.sigmoid(proj[:, 3 * c:])
    acc_a[...] = jnp.zeros_like(acc_a)

    def attend(h):
        logits = nt(k, masked(q, h)) * scale + pb_t[h].astype(F32) + mask_col[...]
        e = jnp.exp(logits - jnp.max(logits, axis=0, keepdims=True))
        prob = e / jnp.sum(e, axis=0, keepdims=True)
        probs[h] = prob
        acc_a[...] += tn(prob.astype(BF16), masked(v, h))
    rows_loop(heads, attend)
    att = acc_a[...]
    gated = (gate * att).astype(BF16)
    s_mid = (s[...].astype(F32) + nn(gated, w_o[...])).astype(BF16)
    m_hat, m_inv = norm_parts(s_mid)
    mid_n = m_hat.astype(BF16)
    width = c
    dsv = ds[...]
    acc_b[...] = jnp.zeros_like(acc_b)
    acc_c[...] = jnp.zeros_like(acc_c)
    for t in range(inner // width):
        at = slice(t * width, (t + 1) * width)
        at2 = slice(inner + t * width, inner + (t + 1) * width)
        h1 = nn(mid_n, w_up[:, at])
        h2 = nn(mid_n, w_up[:, at2])
        sg, si = silu_parts(h1, h2)
        act = (si * h2).astype(BF16)
        acc_b[...] += nn(act, w_down[at, :])
        act_s[:, at] = act
        d_act = round_bf(nt(dsv, w_down[at, :]))
        d1 = (d_act * h2 * (sg + si * (1.0 - sg))).astype(BF16)
        d2 = (d_act * si).astype(BF16)
        dh_s[:, at] = d1
        dh_s[:, at2] = d2
        acc_c[...] += nt(d1, w_up[:, at]) + nt(d2, w_up[:, at2])
    s_new[...] = (s_mid.astype(F32) + acc_b[...]).astype(BF16)
    ds_mid = (dsv.astype(F32) + norm_back(m_hat, m_inv, round_bf(acc_c[...]))).astype(BF16)
    rows_qkvg = c * 4 * c // 128
    off_o = rows_qkvg + c // 128 + pb_t.shape[0]
    off_up = off_o + c * c // 128
    off_down = off_up + c * 2 * inner // 128
    cb = c // 128
    for t in range(2 * inner // c):
        g = tn(mid_n, dh_s[:, t * c:(t + 1) * c])
        for b in range(cb):
            put_rows(grads, off_up, 2 * inner // 128, t * cb + b, g[:, b * 128:(b + 1) * 128])
    for t in range(inner // c):
        g = tn(act_s[:, t * c:(t + 1) * c], dsv)
        for b in range(cb):
            put_rows(grads, off_down + t * c * cb, cb, b, g[:, b * 128:(b + 1) * 128])
    g = tn(gated, ds_mid)
    for b in range(cb):
        put_rows(grads, off_o, cb, b, g[:, b * 128:(b + 1) * 128])

    d_gated = round_bf(nt(ds_mid, w_o[...]))
    d_att = (d_gated * gate).astype(BF16)
    d_gl = (d_gated * att * gate * (1.0 - gate)).astype(BF16)
    acc_a[...] = jnp.zeros_like(acc_a)
    acc_b[...] = jnp.zeros_like(acc_b)
    acc_c[...] = jnp.zeros_like(acc_c)

    def back(h):
        prob = probs[h]
        dam = masked(d_att, h)
        dp = round_bf(nt(v, dam))
        dst = prob * (dp - jnp.sum(prob * dp, axis=0, keepdims=True))
        d_pb[h] = dst.astype(BF16)
        dsb = (dst * scale).astype(BF16)
        acc_a[...] += tn(dsb, masked(k, h))
        acc_b[...] += nn(dsb, masked(q, h))
        acc_c[...] += nn(prob.astype(BF16), dam)
    rows_loop(heads, back)
    parts = [acc_a[...].astype(BF16), acc_b[...].astype(BF16), acc_c[...].astype(BF16), d_gl]
    dn = jnp.zeros((n, c), F32)
    for t in range(4):
        g = tn(normed, parts[t])
        dn = dn + nt(parts[t], w_qkvg[:, t * c:(t + 1) * c])
        for b in range(cb):
            put_rows(grads, 0, 4 * cb, t * cb + b, g[:, b * 128:(b + 1) * 128])
    qb = jnp.sum(parts[0].astype(F32), axis=0, keepdims=True)
    for b in range(cb):
        grads[rows_qkvg + b:rows_qkvg + b + 1, :] = qb[:, b * 128:(b + 1) * 128]
    grads[rows_qkvg + cb:off_o, :] = jnp.zeros((off_o - rows_qkvg - cb, 128), F32)
    ds_in[...] = (ds_mid.astype(F32) + norm_back(s_hat, s_inv, round_bf(dn))).astype(BF16)


def single_track(s, ds, pb_g, mask_col, w_qkvg, q_bias, w_o, w_up, w_down, heads):
    n, c = s.shape
    inner = w_down.shape[0]
    rows = (4 * c * c + c + 128 * heads + c * c + 3 * inner * c) // 128
    outs = [((n, c), BF16), ((n, c), BF16), ((heads, n, n), BF16), ((rows, 128), F32)]
    scratch = [pltpu.VMEM((heads, n, n), BF16), pltpu.VMEM((heads, n, n), F32)] + [pltpu.VMEM((n, c), F32)] * 3 + [
        pltpu.VMEM((n, 2 * inner), BF16), pltpu.VMEM((n, inner), BF16)]
    return call(functools.partial(single_body, heads), outs, scratch, s, ds, pb_g, mask_col, w_qkvg, q_bias, w_o, w_up,
                w_down, name='single_track')


def gather(x):
    return lax.all_gather(x, GROUP_AXIS, axis=0, tiled=False)


def gather_rows(x):
    return lax.all_gather(x, GROUP_AXIS, axis=0, tiled=True)


def exchange(x):
    return lax.all_to_all(x, GROUP_AXIS, 1, 0, tiled=True)


def exchange_back(x):
    return lax.all_to_all(x, GROUP_AXIS, 0, 1, tiled=True)


def reduce_bias(d_bias, heads, group):
    n = d_bias.shape[1]
    parts = d_bias.reshape(heads, group, n // group, n).transpose(1, 0, 2, 3)
    own = lax.psum_scatter(parts, GROUP_AXIS, scatter_dimension=0, tiled=False)
    own = own.astype(BF16).transpose(1, 0, 2)
    return jnp.pad(own, ((0, 0), (0, 16 - heads), (0, 0)))


def pad_bias(w_tb):
    return jnp.pad(w_tb.T, ((0, 16 - w_tb.shape[1]), (0, 0)))


def bias_grad(g_t, heads):
    return g_t[:heads].T.reshape(-1, 128)


def chunk_rows(total, parts):
    shard = total // parts
    return shard, -(-(shard // 128 + 2) // 32) * 32


def reduce_single(grads, n_pair, total):
    parts, group = lax.axis_size(BATCH_AXIS), lax.axis_size(GROUP_AXIS)
    shard, chunk = chunk_rows(total, parts)
    quarter = chunk // group
    q = lax.axis_index(GROUP_AXIS)
    padded = jnp.pad(grads, ((n_pair, chunk), (0, 0)))
    pieces = [lax.dynamic_slice(padded, (d * shard // 128 + q * quarter, 0), (quarter, 128)) for d in range(parts)]
    own = lax.psum_scatter(jnp.concatenate(pieces), BATCH_AXIS, scatter_dimension=0, tiled=True)
    return gather_rows(own)


def finish_grads(own, pair_rows, g_pb, pb_row, total):
    parts, group = lax.axis_size(BATCH_AXIS), lax.axis_size(GROUP_AXIS)
    shard, chunk = chunk_rows(total, parts)
    n_pair, n_pb = pair_rows.shape[0], g_pb.shape[0]
    rows = jnp.concatenate([pair_rows, g_pb])
    rows = jnp.pad(rows, ((0, -rows.shape[0] % (8 * group)), (0, 0)))
    rows = lax.psum_scatter(rows, GROUP_AXIS, scatter_dimension=0, tiled=True)
    rows = gather_rows(lax.psum(rows, BATCH_AXIS))
    first = lax.axis_index(BATCH_AXIS) * shard // 128
    pair = jnp.pad(rows[:n_pair], ((0, 2 * chunk), (0, 0)))
    own = own + lax.dynamic_slice(pair, (jnp.minimum(first, n_pair + chunk), 0), (chunk, 128))
    extra = jnp.pad(rows[n_pair:n_pair + n_pb], ((chunk, chunk), (0, 0)))
    at = jnp.clip(chunk - (pb_row - first), 0, chunk + n_pb)
    own = own + lax.dynamic_slice(extra, (at, 0), (chunk, 128))
    offset = (lax.axis_index(BATCH_AXIS) * shard) % 128
    return lax.dynamic_slice(own.reshape(-1), (offset,), (shard,))


def device_step(single_blk, pair_blk, mask_blk, d_single_blk, d_pair_blk, *weights):
    group = lax.axis_size(GROUP_AXIS)
    me = lax.axis_index(GROUP_AXIS)
    s_rows, z_zero = single_blk[0], pair_blk[0]
    r = z_zero.shape[0]
    mask_bias = (mask_blk.astype(F32) - 1.0) * MASK_PENALTY
    (mo_in, mo_gate, mo_proj, mi_in, mi_gate, mi_proj, st_qkvg, st_tb, st_o, en_qkvg, en_tb, en_o, p_up, p_down,
     g_qkvg, g_qb, g_pb, g_o, g_up, g_down) = weights
    tri_heads, single_heads = st_tb.shape[1], g_pb.shape[1]
    st_t, en_t, pb_t = pad_bias(st_tb), pad_bias(en_tb), g_pb.T
    total = sum(w.size for w in weights)

    both = gather_rows(jnp.stack([s_rows, d_single_blk[0]], axis=1))
    s_all, ds_all = both[:, 0], both[:, 1]
    d_pair_recv = exchange(d_pair_blk[0])

    left1, right1 = mul_pre(z_zero, mo_in, False)
    right1_g = gather(right1)
    z_one, xh1, xhat1, rstd1, _ = mul_post(left1, right1_g, z_zero, mo_gate, mo_proj, st_t, False)
    left1_g = gather(left1)
    left2, right2, left2_nat = mul_pre(z_one, mi_in, True)
    z_two, xh2, xhat2, rstd2, bias3 = mul_post(exchange(left2_nat), gather(right2), z_one, mi_gate, mi_proj, st_t, True)
    bias3_g = gather_rows(bias3)
    z_three = att_fwd(z_two, bias3_g, mask_bias, st_qkvg, st_o, tri_heads)
    zc_three, bias4 = turn(exchange(z_three), en_t)
    bias4_g = gather_rows(bias4)
    zc_four = att_fwd(zc_three, bias4_g, mask_bias, en_qkvg, en_o, tri_heads)
    zc_five, z_five_turn, pbias = pair_trans(zc_four, p_up, p_down, pb_t)
    z_five = exchange_back(z_five_turn)
    s_new, ds_in, d_pb, single_grads = single_track(
        s_all, ds_all, gather_rows(pbias), mask_bias.reshape(-1, 1), g_qkvg, g_qb.reshape(1, -1), g_o, g_up, g_down,
        single_heads)
    n_pair = sum(w.size for w in weights[:14]) // 128
    own_single = reduce_single(single_grads, n_pair, total)
    d_pb_own = lax.dynamic_slice_in_dim(d_pb, me * r, r, 1).transpose(1, 0, 2)
    dzc_four, d_pup, d_pdown, d_pbt = pair_trans_back(d_pair_recv, zc_five, d_pb_own, zc_four, p_up, p_down, pb_t)
    dz_part4, d_bias4, d_enq, d_eno = att_back(dzc_four, zc_three, bias4_g, mask_bias, en_qkvg, en_o, tri_heads)
    n = z_zero.shape[1]
    db4 = reduce_bias(d_bias4.reshape(tri_heads, n, n), tri_heads, group)
    dz_three_turn, d_ent = bias_back(dz_part4, zc_three, db4, en_t, True)
    dz_three = exchange_back(dz_three_turn)
    dz_part3, d_bias3, d_stq, d_sto = att_back(dz_three, z_two, bias3_g, mask_bias, st_qkvg, st_o, tri_heads)
    db3 = reduce_bias(d_bias3.reshape(tri_heads, n, n), tri_heads, group)
    dz_two, d_stt = bias_back(dz_part3, z_two, db3, st_t, False)
    dm2, dgp2, d_mip = mul_back_post(dz_two, z_one, xh2, xhat2, rstd2, mi_gate, mi_proj, False)
    dz_one, d_mii, d_mig = mul_back_pre(dz_two, z_one, dgp2, gather(dm2), left2, right2, mask_bias, mi_in, mi_gate, True)
    dm1, dgp1, d_mop, dm1_nat = mul_back_post(dz_one, z_zero, xh1, xhat1, rstd1, mo_gate, mo_proj, True)
    dz_zero, d_moi, d_mog = mul_back_pre(dz_one, z_zero, dgp1, dm1, exchange(dm1_nat), right1_g, left1_g, mo_in, mo_gate,
                                         False)
    flat = [d_moi, d_mog, d_mop, d_mii, d_mig, d_mip, d_stq, bias_grad(d_stt, tri_heads), d_sto,
            d_enq, bias_grad(d_ent, tri_heads), d_eno, d_pup, d_pdown]
    pair_rows = jnp.concatenate([g.reshape(-1, 128) for g in flat])
    pb_row = n_pair + (g_qkvg.size + g_qb.size) // 128
    grad_flat = finish_grads(own_single, pair_rows, bias_grad(d_pbt, single_heads), pb_row, total)
    s_out = lax.dynamic_slice_in_dim(s_new, me * r, r, 0)
    ds_out = lax.dynamic_slice_in_dim(ds_in, me * r, r, 0)
    return s_out[None], z_five[None], ds_out[None], dz_zero[None], grad_flat


def solution(mesh):
    spec_single = P(BATCH_AXIS, GROUP_AXIS, None)
    spec_pair = P(BATCH_AXIS, GROUP_AXIS, None, None)
    spec_mask = P(BATCH_AXIS, None)

    def block_fn(single_rep, pair_rep, token_mask, d_single_out, d_pair_out, *weights):
        in_specs = (spec_single, spec_pair, spec_mask, spec_single, spec_pair) + tuple(P() for w_item in weights)
        out_specs = (spec_single, spec_pair, spec_single, spec_pair, P(BATCH_AXIS))
        mapped = jax.shard_map(device_step, mesh=mesh, in_specs=in_specs, out_specs=out_specs, check_vma=False)
        return mapped(single_rep, pair_rep, token_mask, d_single_out, d_pair_out, *weights)

    return block_fn
```

```python
import functools
import jax
import jax.numpy as jnp
from jax import lax
from jax.experimental import pallas as pl
from jax.experimental.pallas import tpu as pltpu
from jax.sharding import PartitionSpec as P

BATCH_AXIS = 'dp'
GROUP_AXIS = 'dap'
NORM_EPS = 1e-5
MASK_PENALTY = 1.0e9
ROWS_STEP = 4
CHAN_STEP = 8
INTERPRET = False
COST = pl.CostEstimate(flops=80_000_000, bytes_accessed=4_000_000, transcendentals=0)
BF16 = jnp.bfloat16
LANES = 128
ALL = ...
F32 = jnp.float32


def nn(x, y):
    return lax.dot_general(x, y, (((1,), (0,)), ((), ())), preferred_element_type=F32)


def nt(x, y):
    return lax.dot_general(x, y, (((1,), (1,)), ((), ())), preferred_element_type=F32)


def tn(x, y):
    return lax.dot_general(x, y, (((0,), (0,)), ((), ())), preferred_element_type=F32)


def norm_parts(x):
    xf = x.astype(F32)
    cent = xf - jnp.mean(xf, axis=-1, keepdims=True)
    rstd = lax.rsqrt(jnp.mean(cent * cent, axis=-1, keepdims=True) + NORM_EPS)
    return cent * rstd, rstd


def norm_back(xhat, rstd, dn):
    m1 = jnp.mean(dn, axis=-1, keepdims=True)
    m2 = jnp.mean(dn * xhat, axis=-1, keepdims=True)
    return rstd * (dn - m1 - xhat * m2)


def round_bf(x):
    return x.astype(BF16).astype(F32)


def swap_lead(src, dst):
    steps = src.shape[1] // 16

    def body(t, carry):
        at = pl.ds(pl.multiple_of(t * 16, 16), 16)
        dst[at] = jnp.swapaxes(src[:, at, :], 0, 1)
        return carry
    lax.fori_loop(0, steps, body, 0)


def swap_minor(src, dst, step=4):
    def body(t, carry):
        at = pl.ds(t * step, step)
        dst[at] = jnp.swapaxes(src[at], 1, 2)
        return carry
    lax.fori_loop(0, src.shape[0] // step, body, 0)


def rows_loop(count, body):
    def wrapped(t, carry):
        body(t)
        return carry
    lax.fori_loop(0, count, wrapped, 0)


def call(body, outs, scratch, *args, name):
    outs = [jax.ShapeDtypeStruct(s, d) for s, d in outs]
    return pl.pallas_call(
        body, out_shape=outs, scratch_shapes=scratch, name=name, interpret=INTERPRET,
        in_specs=[pl.BlockSpec(memory_space=pltpu.VMEM)] * len(args),
        out_specs=[pl.BlockSpec(memory_space=pltpu.VMEM)] * len(outs),
        cost_estimate=COST,
        compiler_params=pltpu.CompilerParams(vmem_limit_bytes=56 * 1024 * 1024),
    )(*args)


MESH_IDS = pl.DeviceIdType.MESH
DP_SIZE = 8


def partners():
    me = lax.axis_index(GROUP_AXIS)
    sibling = me + 1 - 2 * (me % 2)
    return me, (sibling, (me + 2) % 4, (sibling + 2) % 4)


def send_views(kind, src, dst, group):
    if kind in ('gather', 'rows'):
        rows = src.shape[0]

        def put(d):
            return dst.at[d] if kind == 'gather' else dst.at[pl.ds(pl.multiple_of(d * rows, rows), rows)]
        return (lambda p: src), put
    if kind in ('parts', 'dp_parts'):
        return (lambda p: src.at[p]), (lambda d: dst.at[d])
    if kind == 'dp_gather':
        return (lambda p: src), (lambda d: dst.at[d])
    if kind == 'cols':
        rows, block = src.shape[0], src.shape[1] // group
        return (lambda p: src.at[:, pl.ds(pl.multiple_of(p * block, block), block)],
                lambda d: dst.at[pl.ds(pl.multiple_of(d * rows, rows), rows)])
    block, cols = src.shape[0] // group, src.shape[1]
    return (lambda p: src.at[pl.ds(pl.multiple_of(p * block, block), block)],
            lambda d: dst.at[:, pl.ds(pl.multiple_of(d * cols, cols), cols)])


def landing(kind, x, group=4):
    if kind == 'gather':
        return (group,) + x.shape
    if kind == 'dp_gather':
        return (DP_SIZE,) + x.shape
    if kind in ('parts', 'dp_parts'):
        return x.shape
    if kind == 'rows':
        return (group * x.shape[0],) + x.shape[1:]
    if kind == 'cols':
        return (group * x.shape[0], x.shape[1] // group) + x.shape[2:]
    return (x.shape[0] // group, group * x.shape[1]) + x.shape[2:]


def dp_partners():
    dp = lax.axis_index(BATCH_AXIS)
    return dp, [(dp + o) % DP_SIZE for o in range(1, DP_SIZE)]


class Transfer:
    def __init__(self, kind, src, dst, sends, recvs, local):
        over_dp = kind.startswith('dp')
        axis = BATCH_AXIS if over_dp else GROUP_AXIS
        me, peers = dp_partners() if over_dp else partners()
        get, put = send_views(kind, src, dst, 4)
        self.relay = kind == 'gather'

        def remote(view, slot, link, to):
            return pltpu.make_async_remote_copy(
                src_ref=view, dst_ref=put(slot), send_sem=sends.at[link], recv_sem=recvs.at[link],
                device_id={axis: to}, device_id_type=MESH_IDS)
        self.own = pltpu.make_async_copy(get(me), put(me), local)
        self.copies = [remote(get(p), me, link, p) for link, p in enumerate(peers[:2] if self.relay else peers)]
        if self.relay:
            self.copies.append(remote(put(peers[1]), peers[1], 2, peers[0]))

    def start(self):
        for c in reversed(self.copies[:2] if self.relay else self.copies):
            c.start()
        self.own.start()

    def forward(self):
        if self.relay:
            self.copies[1].wait_recv()
            self.copies[2].start()

    def wait(self):
        self.forward()
        self.own.wait()
        for link, c in enumerate(self.copies):
            if self.relay and link == 1:
                c.wait_send()
            else:
                c.wait()


def enter(over_dp):
    me, peers = partners()
    barrier = pltpu.get_barrier_semaphore()
    ids = [{GROUP_AXIS: p} for p in peers]
    if over_dp:
        ids += [{BATCH_AXIS: p} for p in dp_partners()[1]]
    for to in ids:
        pl.semaphore_signal(barrier, inc=1, device_id=to, device_id_type=MESH_IDS)
    pl.semaphore_wait(barrier, len(ids))


def call_with(body, moves, outs, scratch, *args, name, cid, late=()):
    count = len(moves)
    lands = [jax.ShapeDtypeStruct(landing(k, x), x.dtype) for k, x in moves]
    n_args, n_outs = len(args), len(outs)

    def whole(*refs):
        srcs, ins = refs[:count], refs[count:count + n_args]
        at = count + n_args
        dsts, results = refs[at:at + count], refs[at + count:at + count + n_outs]
        rest = refs[at + count + n_outs:]
        sends, recvs, local = rest[-3:]
        enter(any(k.startswith('dp') for k, x in moves))
        jobs = [Transfer(moves[m][0], srcs[m], dsts[m], sends.at[m], recvs.at[m], local.at[m]) for m in range(count)]
        for job in jobs:
            job.start()
        for m, job in enumerate(jobs):
            if m not in late:
                job.wait()
        body(*[d for m, d in enumerate(dsts) if m not in late], *ins, *results, *rest[:-3])
        for m in late:
            jobs[m].wait()
    res = pl.pallas_call(
        whole, out_shape=lands + [jax.ShapeDtypeStruct(sh, d) for sh, d in outs], name=name, interpret=INTERPRET,
        in_specs=[pl.BlockSpec(memory_space=pltpu.VMEM)] * (count + n_args),
        out_specs=[pl.BlockSpec(memory_space=pltpu.VMEM)] * (count + n_outs),
        scratch_shapes=list(scratch) + [pltpu.SemaphoreType.DMA((count, DP_SIZE)), pltpu.SemaphoreType.DMA((count, DP_SIZE)),
                                        pltpu.SemaphoreType.DMA((count,))],
        cost_estimate=COST,
        compiler_params=pltpu.CompilerParams(vmem_limit_bytes=60 * 1024 * 1024, collective_id=cid, has_side_effects=True),
    )(*[x for k, x in moves], *args)
    return res[:count], res[count:]


def total_body(g, out, work1, work2, work3, full, recv1, recv2, recv3, recv4, sends, recvs):
    me, peers = partners()
    dp = lax.axis_index(BATCH_AXIS)
    z = dp // 2
    y = dp % 2
    core, x = me % 2, me // 2
    y_peer = {BATCH_AXIS: 2 * z + 1 - y, GROUP_AXIS: me}
    z_peers = [{BATCH_AXIS: ((z + o) % 4) * 2 + y, GROUP_AXIS: me} for o in (1, 2, 3)]
    core_peer = {BATCH_AXIS: dp, GROUP_AXIS: peers[0]}
    x_peer = {BATCH_AXIS: dp, GROUP_AXIS: peers[1]}
    barrier = pltpu.get_barrier_semaphore()
    for p in [core_peer, x_peer, y_peer] + z_peers:
        pl.semaphore_signal(barrier, inc=1, device_id=p, device_id_type=MESH_IDS)
    pl.semaphore_wait(barrier, 6)
    n = g.shape[0]
    half, quarter, eighth = n // 2, n // 4, n // 8

    def part(ref, index, size):
        return ref.at[pl.ds(pl.multiple_of(index * size, size), size)]

    def copy(src, dst, slot, to):
        return pltpu.make_async_remote_copy(src_ref=src, dst_ref=dst, send_sem=sends.at[slot], recv_sem=recvs.at[slot],
                                            device_id=to, device_id_type=MESH_IDS)

    def fold(src, index, size, recv, dst, slot, to):
        c = copy(part(src, 1 - index, size), recv, slot, to)
        c.start()
        c.wait()
        dst[ALL] = part(src, index, size)[ALL] + recv[ALL]
    fold(g, core, half, recv1, work1, 0, core_peer)
    fold(work1, x, quarter, recv2, work2, 1, x_peer)
    fold(work2, y, eighth, recv3, work3, 2, y_peer)
    sent = [copy(work3, recv4.at[o], 3 + o, z_peers[o]) for o in range(3)]
    for c in sent:
        c.start()
    for c in sent:
        c.wait()
    place = core * 4 + x * 2 + y
    part(full, place, eighth)[ALL] = work3[ALL] + recv4[0] + recv4[1] + recv4[2]
    for slot, index, size, to in ((6, place, eighth, y_peer), (7, core * 2 + x, quarter, x_peer),
                                  (8, core, half, core_peer)):
        piece = part(full, index, size)
        c = copy(piece, piece, slot, to)
        c.start()
        c.wait()
    out[ALL] = full[ALL]


def total(g, cid):
    n = g.shape[0]

    def buf(k, lead=()):
        return pltpu.VMEM(lead + (n // k, g.shape[1]), F32)
    return pl.pallas_call(
        total_body, out_shape=jax.ShapeDtypeStruct(g.shape, F32), name='total', interpret=INTERPRET,
        in_specs=[pl.BlockSpec(memory_space=pltpu.VMEM)], out_specs=pl.BlockSpec(memory_space=pltpu.VMEM),
        scratch_shapes=[buf(2), buf(4), buf(8), buf(1), buf(2), buf(4), buf(8), buf(8, (3,)),
                        pltpu.SemaphoreType.DMA((9,)), pltpu.SemaphoreType.DMA((9,))],
        cost_estimate=COST,
        compiler_params=pltpu.CompilerParams(collective_id=cid, has_side_effects=True),
    )(g)


def mul_pre_body(keep_left, z, w_in, *refs):
    if keep_left:
        left_t, right_t, left_nat, sa, sb = refs
    else:
        left_t, right_t, sa, sb = refs
    width = w_in.shape[1] // 4

    def step(t):
        at = pl.ds(t * ROWS_STEP, ROWS_STEP)
        zc = z[at].reshape(-1, z.shape[-1])
        normed = norm_parts(zc)[0].astype(BF16)
        proj = nn(normed, w_in[ALL])
        left = (jax.nn.sigmoid(proj[:, width:2 * width]) * proj[:, :width]).astype(BF16)
        right = (jax.nn.sigmoid(proj[:, 3 * width:]) * proj[:, 2 * width:3 * width]).astype(BF16)
        left = left.reshape(ROWS_STEP, -1, width)
        right = right.reshape(ROWS_STEP, -1, width)
        if keep_left:
            left_nat[at] = left
        sa[at] = jnp.swapaxes(left, 1, 2)
        sb[at] = jnp.swapaxes(right, 1, 2)
    rows_loop(z.shape[0] // ROWS_STEP, step)
    swap_lead(sa, left_t)
    swap_lead(sb, right_t)


def mul_pre(z, w_in, keep_left):
    r, n, c = z.shape
    width = w_in.shape[1] // 4
    outs = [((width, r, n), BF16)] * 2 + ([((r, n, width), BF16)] if keep_left else [])
    scratch = [pltpu.VMEM((r, width, n), BF16)] * 2
    return call(functools.partial(mul_pre_body, keep_left), outs, scratch, z, w_in,
                name='mul_pre_in' if keep_left else 'mul_pre_out')


def joined(ref, ch):
    return jnp.concatenate([ref[dev, ch] for dev in range(ref.shape[0])], axis=0)


def mul_post_body(incoming, *refs):
    if incoming:
        left, right_g, z, w_gate, w_out, w_tb, z_new, xh_nat, xhat, rstd, bias, tb, t2, u1, u2, u3, b1, b2 = refs
    else:
        right_g, left, z, w_gate, w_out, z_new, xh_nat, xhat, rstd, tb, t2 = refs
    width = xhat.shape[0]
    if incoming:
        swap_lead(left, u1)
        swap_minor(u1, u2)
        swap_lead(u2, u3)
        left = u3

    def mix(t):
        for s in range(CHAN_STEP):
            ch = t * CHAN_STEP + s
            if incoming:
                xhat[ch] = nn(left[ch], joined(right_g, ch))
            else:
                xhat[ch] = nt(left[ch], joined(right_g, ch))
    rows_loop(width // CHAN_STEP, mix)
    zero = jnp.zeros(xhat.shape[1:], F32)
    total = lax.fori_loop(0, width, lambda ch, acc: acc + xhat[ch], zero)
    mean = total / width
    sq = lax.fori_loop(0, width, lambda ch, acc: acc + (xhat[ch] - mean) * (xhat[ch] - mean), zero)
    inv = lax.rsqrt(sq / width + NORM_EPS)
    rstd[ALL] = inv

    def scale(ch):
        val = (xhat[ch] - mean) * inv
        xhat[ch] = val
        tb[ch] = val.astype(BF16)
    rows_loop(width, scale)
    swap_lead(tb, t2)

    def step(t):
        at = pl.ds(t * ROWS_STEP, ROWS_STEP)
        zc = z[at].reshape(-1, z.shape[-1])
        xh = jnp.swapaxes(t2[at], 1, 2)
        xh_nat[at] = xh
        normed = norm_parts(zc)[0].astype(BF16)
        gate = jax.nn.sigmoid(nn(normed, w_gate[ALL]))
        upd = gate * nn(xh.reshape(-1, width), w_out[ALL])
        znew = (zc.astype(F32) + upd).astype(BF16)
        z_new[at] = znew.reshape(ROWS_STEP, -1, z.shape[-1])
        if incoming:
            bias_rows(znew, w_tb, b1, t)
    rows_loop(z.shape[0] // ROWS_STEP, step)
    if incoming:
        swap_lead(b1, b2)
        bias[ALL] = b2[:bias.shape[0]]


def bias_rows(zc, w_t, bias, t):
    normed = norm_parts(zc)[0].astype(BF16).reshape(ROWS_STEP, -1, zc.shape[-1])
    for s in range(ROWS_STEP):
        bias[t * ROWS_STEP + s] = nt(w_t[ALL], normed[s]).astype(BF16)


def mul_post(left, right, z, w_gate, w_out, w_tb, heads, incoming, cid):
    r, n, c = z.shape
    width = w_out.shape[0]
    outs = [((r, n, c), BF16), ((r, n, width), BF16), ((width, r, n), F32), ((r, n), F32)]
    scratch = [pltpu.VMEM((width, r, n), BF16), pltpu.VMEM((r, width, n), BF16)]
    if incoming:
        outs.append(((heads, r, n), BF16))
        scratch += [pltpu.VMEM((r, n, width), BF16), pltpu.VMEM((r, width, n), BF16), pltpu.VMEM((width, r, n), BF16),
                    pltpu.VMEM((r, 16, n), BF16), pltpu.VMEM((16, r, n), BF16)]
        moves, args = [('cols', left), ('gather', right)], (z, w_gate, w_out, w_tb)
    else:
        moves, args = [('gather', right)], (left, z, w_gate, w_out)
    return call_with(functools.partial(mul_post_body, incoming), moves, outs, scratch, *args, cid=cid,
                     name='mul_post_in' if incoming else 'mul_post_out')


def mul_back_post_body(want_nat, dz, z, xh_nat, xhat, rstd, w_gate, w_out, d_t, dgp, g_out, *refs):
    if want_nat:
        d_nat, td, td2 = refs
    else:
        td, td2 = refs
    width = xhat.shape[0]
    g_out[ALL] = jnp.zeros_like(g_out)

    def step(t):
        at = pl.ds(t * ROWS_STEP, ROWS_STEP)
        zc = z[at].reshape(-1, z.shape[-1])
        dzf = dz[at].reshape(-1, z.shape[-1]).astype(F32)
        xh = xh_nat[at].reshape(-1, width)
        normed = norm_parts(zc)[0].astype(BF16)
        gate = jax.nn.sigmoid(nn(normed, w_gate[ALL]))
        y = nn(xh, w_out[ALL])
        dgp[at] = (dzf * y * gate * (1.0 - gate)).astype(BF16).reshape(ROWS_STEP, -1, z.shape[-1])
        dy = (dzf * gate).astype(BF16)
        g_out[ALL] += tn(xh, dy)
        dxh = nt(dy, w_out[ALL]).astype(BF16).reshape(ROWS_STEP, -1, width)
        td[at] = jnp.swapaxes(dxh, 1, 2)
    rows_loop(z.shape[0] // ROWS_STEP, step)
    swap_lead(td, td2)
    zero = jnp.zeros(xhat.shape[1:], F32)

    def sums(ch, acc):
        d = td2[ch].astype(F32)
        return acc[0] + d, acc[1] + d * xhat[ch]
    s1, s2 = lax.fori_loop(0, width, sums, (zero, zero))
    s1, s2, inv = s1 / width, s2 / width, rstd[ALL]

    def fin(ch):
        d_t[ch] = (inv * (td2[ch].astype(F32) - s1 - xhat[ch] * s2)).astype(BF16)
    rows_loop(width, fin)
    if want_nat:
        swap_lead(d_t, td)
        swap_minor(td, d_nat)


def mul_back_post(dz, z, xh_nat, xhat, rstd, w_gate, w_out, want_nat, cid, extra):
    r, n, c = z.shape
    width = w_out.shape[0]
    outs = [((width, r, n), BF16), ((r, n, c), BF16), ((width, c), F32)]
    if want_nat:
        outs.append(((r, n, width), BF16))
    scratch = [pltpu.VMEM((r, width, n), BF16), pltpu.VMEM((width, r, n), BF16)]
    return call_with(functools.partial(mul_back_post_body, want_nat), extra, outs, scratch, dz, z, xh_nat, xhat, rstd,
                     w_gate, w_out, cid=cid, name='mul_back_post', late=tuple(range(len(extra))))


def mul_back_pre_body(incoming, moved, dz, z, dgp, opa, opb, opc, w_in, w_gate, dz_in, g_in, g_gate, da_t, db_t, da_r,
                      db_r, *scr):
    width = w_in.shape[1] // 4
    if incoming:
        d_g, left_t, right_t = moved, opa, opb
    else:
        d_t, d_recv, right_g, left_g = opa, moved, opb, opc
        u1, u2, u3 = scr
        swap_lead(d_recv, u1)
        swap_minor(u1, u2)
        swap_lead(u2, u3)

    def mix(t):
        for s in range(CHAN_STEP):
            ch = t * CHAN_STEP + s
            if incoming:
                d_all = joined(d_g, ch)
                da_t[ch] = nt(right_t[ch], d_all).astype(BF16)
                db_t[ch] = nn(left_t[ch], d_all).astype(BF16)
            else:
                da_t[ch] = nn(d_t[ch], joined(right_g, ch)).astype(BF16)
                db_t[ch] = nn(u3[ch], joined(left_g, ch)).astype(BF16)
    rows_loop(width // CHAN_STEP, mix)
    swap_lead(da_t, da_r)
    swap_lead(db_t, db_r)
    g_in[ALL] = jnp.zeros_like(g_in)
    g_gate[ALL] = jnp.zeros_like(g_gate)

    def step(t):
        at = pl.ds(t * ROWS_STEP, ROWS_STEP)
        c = z.shape[-1]
        zc = z[at].reshape(-1, c)
        da = jnp.swapaxes(da_r[at], 1, 2).reshape(-1, width).astype(F32)
        db = jnp.swapaxes(db_r[at], 1, 2).reshape(-1, width).astype(F32)
        zhat, inv = norm_parts(zc)
        normed = zhat.astype(BF16)
        proj = nn(normed, w_in[ALL])
        sa = jax.nn.sigmoid(proj[:, width:2 * width])
        sb = jax.nn.sigmoid(proj[:, 3 * width:])
        dproj = jnp.concatenate([
            (da * sa).astype(BF16), (da * proj[:, :width] * sa * (1.0 - sa)).astype(BF16),
            (db * sb).astype(BF16), (db * proj[:, 2 * width:3 * width] * sb * (1.0 - sb)).astype(BF16)], axis=1)
        dg = dgp[at].reshape(-1, c)
        g_in[ALL] += tn(normed, dproj)
        g_gate[ALL] += tn(normed, dg)
        dn = round_bf(nt(dproj, w_in[ALL]) + nt(dg, w_gate[ALL]))
        out = dz[at].reshape(-1, c).astype(F32) + norm_back(zhat, inv, dn)
        dz_in[at] = out.astype(BF16).reshape(ROWS_STEP, -1, c)
    rows_loop(z.shape[0] // ROWS_STEP, step)


def mul_back_pre(moves, dz, z, dgp, opa, opb, opc, w_in, w_gate, incoming, cid):
    r, n, c = z.shape
    width = w_in.shape[1] // 4
    outs = [((r, n, c), BF16), (w_in.shape, F32), (w_gate.shape, F32)]
    scratch = [pltpu.VMEM((width, r, n), BF16)] * 2 + [pltpu.VMEM((r, width, n), BF16)] * 2
    if not incoming:
        scratch += [pltpu.VMEM((r, n, width), BF16), pltpu.VMEM((r, width, n), BF16), pltpu.VMEM((width, r, n), BF16)]
    return call_with(functools.partial(mul_back_pre_body, incoming), moves, outs, scratch, dz, z, dgp, opa, opb, opc,
                     w_in, w_gate, cid=cid, name='mul_back_pre_in' if incoming else 'mul_back_pre_out',
                     late=tuple(range(1, len(moves))))


def head_masks(width, heads):
    lane = lax.broadcasted_iota(jnp.int32, (1, width), 1)
    size = width // heads
    return [(lane >= h * size) & (lane < (h + 1) * size) for h in range(heads)]


def stack_heads(x, masks):
    zero = jnp.zeros_like(x)
    return jnp.concatenate([jnp.where(m, x, zero) for m in masks], axis=0)


def pick_heads(x, masks):
    n = x.shape[0] // len(masks)
    out = x[:n]
    for h in range(1, len(masks)):
        out = jnp.where(masks[h], x[h * n:(h + 1) * n], out)
    return out


def load_bias(bias_g, bias_s, add_mask, heads):
    group, rows = bias_g.shape[0], bias_g.shape[2]
    for h in range(heads):
        for d in range(group):
            at = (h * group + d) * rows
            bias_s[at:at + rows] = bias_g[d, h].astype(F32) + add_mask


def soft(logits):
    top = jnp.max(logits, axis=-1, keepdims=True)
    e = jnp.exp(logits - top)
    return e / jnp.sum(e, axis=-1, keepdims=True)


def att_body(heads, bias_g, z, mask, w_qkvg, w_o, z_new, bias_s):
    width = w_o.shape[0]
    n = z.shape[1]
    masks = head_masks(width, heads)
    scale = (width // heads) ** -0.5
    load_bias(bias_g, bias_s, mask[ALL], heads)

    def step(t):
        at = pl.ds(t * ROWS_STEP, ROWS_STEP)
        zc = z[at].reshape(-1, z.shape[-1])
        normed = norm_parts(zc)[0].astype(BF16)
        proj = nn(normed, w_qkvg[ALL])
        qkv = proj[:, :3 * width].astype(BF16)
        outs = []
        for s in range(ROWS_STEP):
            row = qkv[s * n:(s + 1) * n]
            q, k, v = row[:, :width], row[:, width:2 * width], row[:, 2 * width:]
            prob = soft(nt(stack_heads(q, masks), k) * scale + bias_s[ALL]).astype(BF16)
            outs.append(pick_heads(nn(prob, v), masks))
        att = jnp.concatenate(outs, axis=0)
        gated = (jax.nn.sigmoid(proj[:, 3 * width:]) * att).astype(BF16)
        out = (zc.astype(F32) + nn(gated, w_o[ALL])).astype(BF16)
        z_new[at] = out.reshape(ROWS_STEP, n, -1)
    rows_loop(z.shape[0] // ROWS_STEP, step)


def att_fwd(z, bias, mask, w_qkvg, w_o, heads, cid, extra):
    n = z.shape[1]
    moves = [('gather', bias)] + extra
    return call_with(functools.partial(att_body, heads), moves, [(z.shape, BF16)], [pltpu.VMEM((heads * n, n), F32)],
                     z, mask, w_qkvg, w_o, cid=cid, name='att_fwd', late=tuple(range(1, len(moves))))


def att_back_body(heads, dz, z, bias_g, mask, w_qkvg, w_o, dz_part, d_bias, g_qkvg, g_o, bias_s):
    width = w_o.shape[0]
    n, c = z.shape[1:]
    masks = head_masks(width, heads)
    scale = (width // heads) ** -0.5
    load_bias(bias_g, bias_s, mask[ALL], heads)
    d_bias[ALL] = jnp.zeros_like(d_bias)
    g_qkvg[ALL] = jnp.zeros_like(g_qkvg)
    g_o[ALL] = jnp.zeros_like(g_o)
    step_rows = 2

    def step(t):
        at = pl.ds(t * step_rows, step_rows)
        zc = z[at].reshape(-1, c)
        dzc = dz[at].reshape(-1, c)
        zhat, inv = norm_parts(zc)
        normed = zhat.astype(BF16)
        proj = nn(normed, w_qkvg[ALL])
        qkv = proj[:, :3 * width].astype(BF16)
        gate = jax.nn.sigmoid(proj[:, 3 * width:])
        d_gated = round_bf(nt(dzc, w_o[ALL]))
        d_att = (d_gated * gate).astype(BF16)
        atts, dprojs = [], []
        for s in range(step_rows):
            row = qkv[s * n:(s + 1) * n]
            q, k, v = row[:, :width], row[:, width:2 * width], row[:, 2 * width:]
            qs = stack_heads(q, masks)
            prob = soft(nt(qs, k) * scale + bias_s[ALL])
            prob_b = prob.astype(BF16)
            att = pick_heads(nn(prob_b, v), masks)
            das = stack_heads(d_att[s * n:(s + 1) * n], masks)
            dp = round_bf(nt(das, v))
            ds = prob * (dp - jnp.sum(prob * dp, axis=-1, keepdims=True))
            d_bias[ALL] += ds
            dsb = (ds * scale).astype(BF16)
            dq = pick_heads(nn(dsb, k), masks)
            dk = tn(dsb, qs)
            dv = tn(prob_b, das)
            atts.append(att)
            dprojs.append(jnp.concatenate([dq.astype(BF16), dk.astype(BF16), dv.astype(BF16)], axis=1))
        att = jnp.concatenate(atts, axis=0)
        d_gl = (d_gated * att * gate * (1.0 - gate)).astype(BF16)
        gated = (gate * att).astype(BF16)
        dproj = jnp.concatenate([jnp.concatenate(dprojs, axis=0), d_gl], axis=1)
        g_o[ALL] += tn(gated, dzc)
        g_qkvg[ALL] += tn(normed, dproj)
        dn = round_bf(nt(dproj, w_qkvg[ALL]))
        out = dzc.astype(F32) + norm_back(zhat, inv, dn)
        dz_part[at] = out.reshape(step_rows, n, c)
    rows_loop(z.shape[0] // step_rows, step)


def att_back(dz, z, bias_g, mask, w_qkvg, w_o, heads, cid, turned, extra):
    n = z.shape[1]
    outs = [(z.shape, F32), ((heads * n, n), F32), (w_qkvg.shape, F32), (w_o.shape, F32)]
    body, scratch = functools.partial(att_back_body, heads), [pltpu.VMEM((heads * n, n), F32)]
    moves, args = ([('back', dz)], ()) if turned else ([], (dz,))
    late = tuple(range(len(moves), len(moves) + len(extra)))
    return call_with(body, moves + extra, outs, scratch, *args, z, bias_g, mask, w_qkvg, w_o, cid=cid, name='att_back',
                     late=late)


def bias_back_rows(zc, db, w_t, g_t, t):
    zhat, inv = norm_parts(zc)
    normed = zhat.astype(BF16).reshape(ROWS_STEP, -1, zc.shape[-1])
    dns = []
    for s in range(ROWS_STEP):
        d = db[t * ROWS_STEP + s]
        dns.append(tn(d, w_t[ALL]))
        g_t[ALL] += nn(d, normed[s])
    return norm_back(zhat, inv, round_bf(jnp.concatenate(dns, axis=0)))


def bias_back_body(swap_out, parts, dz_part, z, w_t, dz, g_t, wide, db, *scr):
    g_t[ALL] = jnp.zeros_like(g_t)
    dst = scr[0] if swap_out else dz
    heads = parts.shape[0] // 4
    wide[ALL] = jnp.zeros_like(wide)
    for h in range(heads):
        wide[h] = (parts[h] + parts[heads + h] + parts[2 * heads + h] + parts[3 * heads + h]).astype(BF16)
    swap_lead(wide, db)

    def step(t):
        at = pl.ds(t * ROWS_STEP, ROWS_STEP)
        c = z.shape[-1]
        add = bias_back_rows(z[at].reshape(-1, c), db, w_t, g_t, t)
        dst[at] = (dz_part[at].reshape(-1, c) + add).astype(BF16).reshape(ROWS_STEP, -1, c)
    rows_loop(z.shape[0] // ROWS_STEP, step)
    if swap_out:
        swap_lead(scr[0], dz)


def bias_back(d_bias, dz_part, z, w_t, heads, swap_out, cid):
    r, n, c = z.shape
    out = (n, r, c) if swap_out else (r, n, c)
    scratch = [pltpu.VMEM((16, r, n), BF16), pltpu.VMEM((r, 16, n), BF16)]
    if swap_out:
        scratch.append(pltpu.VMEM((r, n, c), BF16))
    return call_with(functools.partial(bias_back_body, swap_out), [('cols', d_bias.reshape(heads, n, n))],
                     [(out, BF16), (w_t.shape, F32)], scratch, dz_part, z, w_t, cid=cid, name='bias_back')[1]


def turn_body(recv, w_t, z_cols, bias, b1, b2):
    swap_lead(recv, z_cols)

    def step(t):
        zc = z_cols[pl.ds(t * ROWS_STEP, ROWS_STEP)].reshape(-1, z_cols.shape[-1])
        bias_rows(zc, w_t, b1, t)
    rows_loop(z_cols.shape[0] // ROWS_STEP, step)
    swap_lead(b1, b2)
    bias[ALL] = b2[:bias.shape[0]]


def turn(z, w_t, heads, cid):
    r, n, c = z.shape
    scratch = [pltpu.VMEM((r, 16, n), BF16), pltpu.VMEM((16, r, n), BF16)]
    return call_with(turn_body, [('cols', z)], [((r, n, c), BF16), ((heads, r, n), BF16)], scratch, w_t, cid=cid,
                     name='turn')[1]


def pair_trans_body(z, w_up, w_down, w_t, z_new, z_turn, bias):
    inner = w_down.shape[0]

    def step(t):
        at = pl.ds(t * ROWS_STEP, ROWS_STEP)
        zc = z[at].reshape(-1, z.shape[-1])
        normed = norm_parts(zc)[0].astype(BF16)
        hid = nn(normed, w_up[ALL])
        acted = (jax.nn.silu(hid[:, :inner]) * hid[:, inner:]).astype(BF16)
        out = (zc.astype(F32) + nn(acted, w_down[ALL])).astype(BF16)
        z_new[at] = out.reshape(ROWS_STEP, -1, z.shape[-1])
        bias_rows(out, w_t, bias, t)
    rows_loop(z.shape[0] // ROWS_STEP, step)
    swap_lead(z_new, z_turn)


def pair_trans(z, w_up, w_down, w_t):
    r, n, c = z.shape
    return call(pair_trans_body, [((r, n, c), BF16), ((n, r, c), BF16), ((r, 16, n), BF16)], [],
                z, w_up, w_down, w_t, name='pair_trans')


def silu_parts(h1, h2):
    sg = jax.nn.sigmoid(h1)
    return sg, h1 * sg


def pair_trans_back_body(d_recv, z5, db, z, w_up, w_down, w_t, dz_in, g_up, g_down, g_t, dz5):
    inner = w_down.shape[0]
    g_up[ALL] = jnp.zeros_like(g_up)
    g_down[ALL] = jnp.zeros_like(g_down)
    g_t[ALL] = jnp.zeros_like(g_t)
    swap_lead(d_recv, dz5)

    def step(t):
        at = pl.ds(t * ROWS_STEP, ROWS_STEP)
        c = z.shape[-1]
        add = bias_back_rows(z5[at].reshape(-1, c), db, w_t, g_t, t)
        dzc = (dz5[at].reshape(-1, c).astype(F32) + add).astype(BF16)
        zhat, inv = norm_parts(z[at].reshape(-1, c))
        normed = zhat.astype(BF16)
        hid = nn(normed, w_up[ALL])
        h1, h2 = hid[:, :inner], hid[:, inner:]
        sg, si = silu_parts(h1, h2)
        acted = (si * h2).astype(BF16)
        d_act = round_bf(nt(dzc, w_down[ALL]))
        d1 = (d_act * h2 * (sg + si * (1.0 - sg))).astype(BF16)
        d2 = (d_act * si).astype(BF16)
        dh = jnp.concatenate([d1, d2], axis=1)
        g_down[ALL] += tn(acted, dzc)
        g_up[ALL] += tn(normed, dh)
        dn = round_bf(nt(dh, w_up[ALL]))
        out = dzc.astype(F32) + norm_back(zhat, inv, dn)
        dz_in[at] = out.astype(BF16).reshape(ROWS_STEP, -1, c)
    rows_loop(z.shape[0] // ROWS_STEP, step)


def pair_trans_back(d_recv, z5, db, z, w_up, w_down, w_t):
    r, n, c = z.shape
    outs = [((r, n, c), BF16), (w_up.shape, F32), (w_down.shape, F32), (w_t.shape, F32)]
    return call(pair_trans_back_body, outs, [pltpu.VMEM((r, n, c), BF16)], d_recv, z5, db, z, w_up, w_down, w_t,
                name='pair_trans_back')


def put_rows(out, first, blocks, block, value):
    out[pl.ds(first + block, value.shape[0], stride=blocks), :] = value


def single_body(heads, pb_g, s, ds, mask_col, w_qkvg, q_bias, w_o, w_up, w_down, s_new, ds_in, d_pb, grads,
                pb_t, probs, acc_a, acc_b, acc_c, dh_s, act_s):
    c = s.shape[1]
    n = s.shape[0]
    inner = w_down.shape[0]
    size = c // heads
    scale = size ** -0.5
    lane = lax.broadcasted_iota(jnp.int32, (1, c), 1)
    swap_lead(pb_g, pb_t)

    def masked(x, h):
        return jnp.where((lane >= h * size) & (lane < (h + 1) * size), x, jnp.zeros_like(x))

    s_hat, s_inv = norm_parts(s[ALL])
    normed = s_hat.astype(BF16)
    proj = nn(normed, w_qkvg[ALL])
    q = (proj[:, :c] + q_bias[ALL].astype(F32)).astype(BF16)
    k = proj[:, c:2 * c].astype(BF16)
    v = proj[:, 2 * c:3 * c].astype(BF16)
    gate = jax.nn.sigmoid(proj[:, 3 * c:])
    acc_a[ALL] = jnp.zeros_like(acc_a)

    def attend(h):
        logits = nt(k, masked(q, h)) * scale + pb_t[h].astype(F32) + mask_col[ALL]
        e = jnp.exp(logits - jnp.max(logits, axis=0, keepdims=True))
        prob = e / jnp.sum(e, axis=0, keepdims=True)
        probs[h] = prob
        acc_a[ALL] += tn(prob.astype(BF16), masked(v, h))
    rows_loop(heads, attend)
    att = acc_a[ALL]
    gated = (gate * att).astype(BF16)
    s_mid = (s[ALL].astype(F32) + nn(gated, w_o[ALL])).astype(BF16)
    m_hat, m_inv = norm_parts(s_mid)
    mid_n = m_hat.astype(BF16)
    width = c
    dsv = ds[ALL]
    acc_b[ALL] = jnp.zeros_like(acc_b)
    acc_c[ALL] = jnp.zeros_like(acc_c)
    for t in range(inner // width):
        at = slice(t * width, (t + 1) * width)
        at2 = slice(inner + t * width, inner + (t + 1) * width)
        h1 = nn(mid_n, w_up[:, at])
        h2 = nn(mid_n, w_up[:, at2])
        sg, si = silu_parts(h1, h2)
        act = (si * h2).astype(BF16)
        acc_b[ALL] += nn(act, w_down[at, :])
        act_s[:, at] = act
        d_act = round_bf(nt(dsv, w_down[at, :]))
        d1 = (d_act * h2 * (sg + si * (1.0 - sg))).astype(BF16)
        d2 = (d_act * si).astype(BF16)
        dh_s[:, at] = d1
        dh_s[:, at2] = d2
        acc_c[ALL] += nt(d1, w_up[:, at]) + nt(d2, w_up[:, at2])
    s_new[ALL] = (s_mid.astype(F32) + acc_b[ALL]).astype(BF16)
    ds_mid = (dsv.astype(F32) + norm_back(m_hat, m_inv, round_bf(acc_c[ALL]))).astype(BF16)
    rows_qkvg = c * 4 * c // LANES
    off_o = rows_qkvg + c // LANES + pb_t.shape[0]
    off_up = off_o + c * c // LANES
    off_down = off_up + c * 2 * inner // LANES
    cb = c // LANES
    for t in range(2 * inner // c):
        g = tn(mid_n, dh_s[:, t * c:(t + 1) * c])
        for b in range(cb):
            put_rows(grads, off_up, 2 * inner // LANES, t * cb + b, g[:, b * LANES:(b + 1) * LANES])
    for t in range(inner // c):
        g = tn(act_s[:, t * c:(t + 1) * c], dsv)
        for b in range(cb):
            put_rows(grads, off_down + t * c * cb, cb, b, g[:, b * LANES:(b + 1) * LANES])
    g = tn(gated, ds_mid)
    for b in range(cb):
        put_rows(grads, off_o, cb, b, g[:, b * LANES:(b + 1) * LANES])

    d_gated = round_bf(nt(ds_mid, w_o[ALL]))
    d_att = (d_gated * gate).astype(BF16)
    d_gl = (d_gated * att * gate * (1.0 - gate)).astype(BF16)
    acc_a[ALL] = jnp.zeros_like(acc_a)
    acc_b[ALL] = jnp.zeros_like(acc_b)
    acc_c[ALL] = jnp.zeros_like(acc_c)

    def back(h):
        prob = probs[h]
        dam = masked(d_att, h)
        dp = round_bf(nt(v, dam))
        dst = prob * (dp - jnp.sum(prob * dp, axis=0, keepdims=True))
        d_pb[h] = dst.astype(BF16)
        dsb = (dst * scale).astype(BF16)
        acc_a[ALL] += tn(dsb, masked(k, h))
        acc_b[ALL] += nn(dsb, masked(q, h))
        acc_c[ALL] += nn(prob.astype(BF16), dam)
    rows_loop(heads, back)
    parts = [acc_a[ALL].astype(BF16), acc_b[ALL].astype(BF16), acc_c[ALL].astype(BF16), d_gl]
    dn = jnp.zeros((n, c), F32)
    for t in range(4):
        g = tn(normed, parts[t])
        dn = dn + nt(parts[t], w_qkvg[:, t * c:(t + 1) * c])
        for b in range(cb):
            put_rows(grads, 0, 4 * cb, t * cb + b, g[:, b * LANES:(b + 1) * LANES])
    qb = jnp.sum(parts[0].astype(F32), axis=0, keepdims=True)
    for b in range(cb):
        grads[rows_qkvg + b:rows_qkvg + b + 1, :] = qb[:, b * LANES:(b + 1) * LANES]
    grads[rows_qkvg + cb:off_o, :] = jnp.zeros((off_o - rows_qkvg - cb, LANES), F32)
    ds_in[ALL] = (ds_mid.astype(F32) + norm_back(s_hat, s_inv, round_bf(dn))).astype(BF16)


def single_track(s, ds, pbias, extra, mask_col, w_qkvg, q_bias, w_o, w_up, w_down, heads, cid):
    n, c = s.shape
    inner = w_down.shape[0]
    rows = (4 * c * c + c + LANES * heads + c * c + 3 * inner * c) // LANES
    outs = [((n, c), BF16), ((n, c), BF16), ((heads, n, n), BF16), ((rows, LANES), F32)]
    scratch = [pltpu.VMEM((heads, n, n), BF16), pltpu.VMEM((heads, n, n), F32)] + [pltpu.VMEM((n, c), F32)] * 3 + [
        pltpu.VMEM((n, 2 * inner), BF16), pltpu.VMEM((n, inner), BF16)]
    moves = [('rows', pbias)] + extra
    return call_with(functools.partial(single_body, heads), moves, outs, scratch, s, ds, mask_col, w_qkvg, q_bias, w_o,
                     w_up, w_down, cid=cid, name='single_track', late=tuple(range(1, len(moves))))


def pad_bias(w_tb):
    return jnp.pad(w_tb.T, ((0, 16 - w_tb.shape[1]), (0, 0)))


def bias_grad(g_t, heads):
    return g_t[:heads].T.reshape(-1, LANES)


def chunk_rows(total, parts):
    shard = total // parts
    return shard, -(-(shard // LANES + 2) // 32) * 32


def single_pieces(grads, n_pair, total_size):
    group = lax.axis_size(GROUP_AXIS)
    shard, chunk = chunk_rows(total_size, DP_SIZE)
    quarter = chunk // group
    q = lax.axis_index(GROUP_AXIS)
    padded = jnp.pad(grads, ((n_pair, chunk), (0, 0)))
    return jnp.stack([lax.dynamic_slice(padded, (d * shard // LANES + q * quarter, 0), (quarter, LANES))
                      for d in range(DP_SIZE)])


def group_parts(grads):
    rows = flat_rows(grads)
    unit = 8 * DP_SIZE * lax.axis_size(GROUP_AXIS)
    rows = jnp.pad(rows, ((0, -rows.shape[0] % unit), (0, 0)))
    return rows.reshape(lax.axis_size(GROUP_AXIS), -1, LANES)


def owner_parts(landed):
    return jnp.sum(landed, axis=0).reshape(DP_SIZE, -1, LANES)


def finish_grads(own, late, early, n_pair, n_pb, pb_row, total_size):
    parts = lax.axis_size(BATCH_AXIS)
    shard, chunk = chunk_rows(total_size, parts)
    first = lax.axis_index(BATCH_AXIS) * shard // LANES
    n_late = late.shape[0]
    n_early = n_pair - n_late
    pair = jnp.concatenate([late, early[:n_early], jnp.zeros((2 * chunk, LANES), F32)])
    own = own + lax.dynamic_slice(pair, (jnp.minimum(first, n_pair + chunk), 0), (chunk, LANES))
    extra = jnp.pad(early[n_early:n_early + n_pb], ((chunk, chunk), (0, 0)))
    at = jnp.clip(chunk - (pb_row - first), 0, chunk + n_pb)
    own = own + lax.dynamic_slice(extra, (at, 0), (chunk, LANES))
    offset = (lax.axis_index(BATCH_AXIS) * shard) % LANES
    return lax.dynamic_slice(own.reshape(-1), (offset,), (shard,))


def flat_rows(grads):
    return jnp.concatenate([g.reshape(-1, LANES) for g in grads])


def device_step(single_blk, pair_blk, mask_blk, d_single_blk, d_pair_blk, *weights):
    me = lax.axis_index(GROUP_AXIS)
    s_rows, z_zero = single_blk[0], pair_blk[0]
    r = z_zero.shape[0]
    mask = (mask_blk.astype(F32) - 1.0) * MASK_PENALTY
    (mo_in, mo_gate, mo_proj, mi_in, mi_gate, mi_proj, st_qkvg, st_tb, st_o, en_qkvg, en_tb, en_o, p_up, p_down,
     g_qkvg, g_qb, g_pb, g_o, g_up, g_down) = weights
    heads, single_heads = st_tb.shape[1], g_pb.shape[1]
    st_t, en_t, pb_t = pad_bias(st_tb), pad_bias(en_tb), g_pb.T
    total_size = sum(w.size for w in weights)

    left1, right1 = mul_pre(z_zero, mo_in, False)
    (right1_g,), (z_one, xh1, xhat1, rstd1) = mul_post(left1, right1, z_zero, mo_gate, mo_proj, None, heads, False, 0)
    left2, right2, left2_nat = mul_pre(z_one, mi_in, True)
    _, (z_two, xh2, xhat2, rstd2, bias3) = mul_post(left2_nat, right2, z_one, mi_gate, mi_proj, st_t, heads, True, 1)
    half = left1.shape[0] // 2
    (bias3_g, s_all, ds_all, left1_lo), (z_three,) = att_fwd(
        z_two, bias3, mask, st_qkvg, st_o, heads, 2,
        [('rows', s_rows), ('rows', d_single_blk[0]), ('gather', left1[:half])])
    zc_three, bias4 = turn(z_three, en_t, heads, 3)
    (bias4_g, left1_hi), (zc_four,) = att_fwd(zc_three, bias4, mask, en_qkvg, en_o, heads, 4, [('gather', left1[half:])])
    zc_five, z_five_turn, pbias = pair_trans(zc_four, p_up, p_down, pb_t)
    (_, z_five, d_pair_recv), (s_new, ds_in, d_pb, single_grads) = single_track(
        s_all, ds_all, pbias, [('back', z_five_turn), ('cols', d_pair_blk[0])], mask.reshape(-1, 1), g_qkvg,
        g_qb.reshape(1, -1), g_o, g_up, g_down, single_heads, 5)
    n_pair = sum(w.size for w in weights[:14]) // LANES
    pieces = single_pieces(single_grads, n_pair, total_size)
    cut = pieces.shape[1] // 2
    d_pb_own = lax.dynamic_slice_in_dim(d_pb, me * r, r, 1).transpose(1, 0, 2)
    dzc_four, d_pup, d_pdown, d_pbt = pair_trans_back(d_pair_recv, zc_five, d_pb_own, zc_four, p_up, p_down, pb_t)
    (own_lo,), (dz_part4, d_bias4, d_enq, d_eno) = att_back(
        dzc_four, zc_three, bias4_g, mask, en_qkvg, en_o, heads, 12, False, [('dp_parts', pieces[:, :cut])])
    dz_three_turn, d_ent = bias_back(d_bias4, dz_part4, zc_three, en_t, heads, True, 6)
    grads_en = [d_enq, bias_grad(d_ent, heads), d_eno, d_pup, d_pdown, bias_grad(d_pbt, single_heads)]
    (_, own_hi, en_mine), (dz_part3, d_bias3, d_stq, d_sto) = att_back(
        dz_three_turn, z_two, bias3_g, mask, st_qkvg, st_o, heads, 7, True,
        [('dp_parts', pieces[:, cut:]), ('parts', group_parts(grads_en))])
    dz_two, d_stt = bias_back(d_bias3, dz_part3, z_two, st_t, heads, False, 8)
    grads_st = [d_stq, bias_grad(d_stt, heads), d_sto]
    own_single = jnp.concatenate([jnp.sum(own_lo, axis=0), jnp.sum(own_hi, axis=0)])
    (own_all, en_own, st_mine), (dm2, dgp2, d_mip) = mul_back_post(
        dz_two, z_one, xh2, xhat2, rstd2, mi_gate, mi_proj, False, 13,
        [('gather', own_single), ('dp_parts', owner_parts(en_mine)), ('parts', group_parts(grads_st))])
    (_, en_quarter, st_own), (dz_one, d_mii, d_mig) = mul_back_pre(
        [('gather', dm2), ('dp_gather', jnp.sum(en_own, axis=0)), ('dp_parts', owner_parts(st_mine))],
        dz_two, z_one, dgp2, left2, right2, mask, mi_in, mi_gate, True, 9)
    (en_all, st_quarter), (dm1, dgp1, d_mop, dm1_nat) = mul_back_post(
        dz_one, z_zero, xh1, xhat1, rstd1, mo_gate, mo_proj, True, 14,
        [('gather', en_quarter.reshape(-1, LANES)), ('dp_gather', jnp.sum(st_own, axis=0))])
    left1_g = jnp.concatenate([left1_lo, left1_hi], axis=1)
    (_, st_all), (dz_zero, d_moi, d_mog) = mul_back_pre(
        [('cols', dm1_nat), ('gather', st_quarter.reshape(-1, LANES))],
        dz_one, z_zero, dgp1, dm1, right1_g, left1_g, mo_in, mo_gate, False, 10)
    late = total(flat_rows([d_moi, d_mog, d_mop, d_mii, d_mig, d_mip]), 11)
    n_st, n_en = sum(w.size for w in weights[6:9]) // LANES, sum(w.size for w in weights[9:14]) // LANES
    early = jnp.concatenate([st_all.reshape(-1, LANES)[:n_st], en_all.reshape(-1, LANES)[:n_en + single_heads]])
    own_single = own_all.reshape(-1, LANES)
    pb_row = n_pair + (g_qkvg.size + g_qb.size) // LANES
    grad_flat = finish_grads(own_single, late, early, n_pair, single_heads, pb_row, total_size)
    s_out = lax.dynamic_slice_in_dim(s_new, me * r, r, 0)
    ds_out = lax.dynamic_slice_in_dim(ds_in, me * r, r, 0)
    return s_out[None], z_five[None], ds_out[None], dz_zero[None], grad_flat


def solution(mesh):
    spec_single = P(BATCH_AXIS, GROUP_AXIS, None)
    spec_pair = P(BATCH_AXIS, GROUP_AXIS, None, None)
    spec_mask = P(BATCH_AXIS, None)

    def block_fn(single_rep, pair_rep, token_mask, d_single_out, d_pair_out, *weights):
        in_specs = (spec_single, spec_pair, spec_mask, spec_single, spec_pair) + tuple(P() for w_item in weights)
        out_specs = (spec_single, spec_pair, spec_single, spec_pair, P(BATCH_AXIS))
        mapped = jax.shard_map(device_step, mesh=mesh, in_specs=in_specs, out_specs=out_specs, check_vma=False)
        return mapped(single_rep, pair_rep, token_mask, d_single_out, d_pair_out, *weights)

    return block_fn
```
